256 devices in a mesh: dp: 256 (over z, y, x, core).
Axes of the slice: x: 4, y: 4, z: 8, core: 2. Of those that a mesh axis runs over, the one named last changes fastest.
Arguments:
- tokens: bfloat16 [262144, 1024], P('dp'), may hold values from -80 to 80
- seg_ids: int32 [256, 1024], P('dp'), may hold values from 0 to 3, as said below
- counts: int32 [256], replicated, may hold values from 1 to 4, as said below
- positives: int32 [1024], P('dp'), may hold values from 0 to 1023, as said below
- w_qkv: bfloat16 [1024, 1536], replicated, may hold values from -0.1875 to 0.1875
- w_out: bfloat16 [512, 1024], replicated, may hold values from -0.25 to 0.25
- ln_gain: float32 [1024], replicated, may hold values from 0.1 to 1.9
- w_proj: bfloat16 [1024, 2048], replicated, may hold values from -0.1875 to 0.1875
Outputs:
- loss: float32 [1024], P('dp')
- grad_pooled: float32 [1024, 1024], P('dp')
The draws below stay inside these ranges and needn't reach their ends.
Inputs may be any that keep to these rules, and one draw needn't show every extreme that they name: `seg_ids`: within a rank, the ids never fall and every id from 0 to 3 occurs. Rank r's live segments are its slots 0 to counts[r] - 1; the other slots hold padding; some rank has all 4 live. `positives`: a live slot of another rank, as rank times 4 plus slot.
All inputs are finite; a program needn't handle non-finite values.
Results may differ from the reference program's by a relative error of at most 0.008.
Values may be sent and summed in bfloat16 or wider, within the bound.
A program may use at most 192 MiB of HBM per device.

```python
import jax
import jax.numpy as jnp
from jax import lax

D = 1024
HEADS = 8
HEAD_DIM = 64
EMBED = 2048
TOK_DEV = 1024
SEG_DEV = 4
TOKENS = 262144
NKEYS = 1024
N_DP = 256


def segment_plan(key):
    key = jax.random.fold_in(key, 7)
    key_count, key_full, key_rank, key_pick, key_length = jax.random.split(key, 5)
    counts = jax.random.randint(key_count, (N_DP,), 1, SEG_DEV + 1, dtype=jnp.int32)
    full_rank = jax.random.randint(key_full, (), 0, N_DP, dtype=jnp.int32)
    counts = jnp.where(jnp.arange(N_DP, dtype=jnp.int32) == full_rank, SEG_DEV, counts).astype(jnp.int32)
    owner = jnp.repeat(jnp.arange(N_DP, dtype=jnp.int32), SEG_DEV)
    offset = jax.random.randint(key_rank, (NKEYS,), 1, N_DP, dtype=jnp.int32)
    target_rank = (owner + offset) % N_DP
    picks = jax.random.randint(key_pick, (NKEYS,), 0, 1048576, dtype=jnp.int32)
    target_slot = picks % counts[target_rank]
    positives = (target_rank * SEG_DEV + target_slot).astype(jnp.int32)
    length_weights = jax.random.randint(key_length, (N_DP, SEG_DEV), 1, 3, dtype=jnp.int32)
    cumulative = jnp.cumsum(length_weights, axis=1).astype(jnp.int32)
    total = cumulative[:, -1:]
    ends = (TOK_DEV - SEG_DEV) * cumulative // total
    starts = ends[:, :-1] + jnp.arange(1, SEG_DEV, dtype=jnp.int32)[None, :]
    position = jnp.arange(TOK_DEV, dtype=jnp.int32)
    segment = jnp.sum((position[None, :, None] >= starts[:, None, :]).astype(jnp.int32), axis=2)
    return (counts, positives, segment.astype(jnp.int32))


def draw_tokens(key, part):
    counts, positives, segment = segment_plan(key)
    key_base = jax.random.fold_in(key, 0)
    key_basis = jax.random.fold_in(key, 3)
    values = jnp.clip(jax.random.normal(key_base, (TOKENS, D), jnp.float32), -6.0, 6.0)
    basis = jnp.clip(jax.random.normal(key_basis, (NKEYS, D), jnp.float32), -4.0, 4.0)
    direction = basis + jnp.take(basis, positives, axis=0)
    slot_of = (jnp.arange(N_DP, dtype=jnp.int32)[:, None] * SEG_DEV + segment).reshape(TOKENS)
    values = values + jnp.take(direction, slot_of, axis=0)
    values = jnp.clip(values, -80.0, 80.0)
    return values.astype(jnp.bfloat16)


def draw_seg_ids(key, part):
    return segment_plan(key)[2]


def draw_counts(key, part):
    return segment_plan(key)[0]


def draw_positives(key, part):
    return segment_plan(key)[1]


def gaussian(own_key, shape, spread, limit, kind=jnp.bfloat16):
    drawn = jax.random.normal(own_key, shape, jnp.float32) * spread
    return jnp.minimum(jnp.maximum(drawn, -limit), limit).astype(kind)


def setup_inputs(seed: int = 0) -> dict:
    key_list = jax.random.split(jax.random.key(seed), 9)
    return {
        "tokens": draw_tokens(jax.random.fold_in(key_list[8], 71), 0),
        "seg_ids": draw_seg_ids(jax.random.fold_in(key_list[8], 71), 0),
        "counts": draw_counts(jax.random.fold_in(key_list[8], 71), 0),
        "positives": draw_positives(jax.random.fold_in(key_list[8], 71), 0),
        "w_qkv": gaussian(key_list[4], (D, 3 * HEADS * HEAD_DIM), D ** -0.5, 0.1875),
        "w_out": gaussian(key_list[5], (HEADS * HEAD_DIM, D), (HEADS * HEAD_DIM) ** -0.5, 0.25),
        "ln_gain": jnp.clip(1.0 + 0.18 * jax.random.normal(key_list[6], (D,), jnp.float32), 0.1, 1.9),
        "w_proj": gaussian(key_list[7], (D, EMBED), D ** -0.5, 0.1875),
    }


logit_scale = 20.0

def attend(tok_rows, segment, w_qkv, w_out, ln_gain):
    rows = tok_rows.shape[0]
    width = w_out.shape[0]
    head_dim = width // HEADS
    qkv = jnp.dot(tok_rows, w_qkv, preferred_element_type=jnp.float32).astype(jnp.bfloat16)
    qkv = qkv.reshape(rows, 3, HEADS, head_dim).astype(jnp.float32)
    scores = jnp.einsum('qhd,khd->hqk', qkv[:, 0], qkv[:, 1]) * head_dim ** (-0.5)
    same = segment[:, None] == segment[None, :]
    scores = jnp.where(same[None], scores, -1e+30)
    row_max = lax.optimization_barrier(jnp.max(scores, axis=-1, keepdims=True))
    exp_scores = jnp.exp(scores - row_max)
    probs = (exp_scores / lax.optimization_barrier(jnp.sum(exp_scores, axis=-1, keepdims=True))).astype(jnp.bfloat16)
    context = jnp.einsum('hqk,khd->qhd', probs.astype(jnp.float32), qkv[:, 2])
    context = context.astype(jnp.bfloat16).reshape(rows, width)
    resid = tok_rows.astype(jnp.float32) + jnp.dot(context, w_out, preferred_element_type=jnp.float32)
    centre = resid - lax.optimization_barrier(jnp.mean(resid, axis=-1, keepdims=True))
    variance = lax.optimization_barrier(jnp.mean(centre * centre, axis=-1, keepdims=True))
    return (centre * lax.rsqrt(variance + 1e-05) * ln_gain).astype(jnp.bfloat16)

def pool_rows(hidden, segment, slots):
    member = jnp.arange(slots, dtype=jnp.int32)[:, None] == segment[None, :]
    sums = jnp.dot(member.astype(jnp.bfloat16), hidden, preferred_element_type=jnp.float32)
    sizes = lax.optimization_barrier(jnp.sum(member.astype(jnp.float32), axis=1, keepdims=True))
    return (sums / sizes).astype(jnp.bfloat16)

def embed_rows(pooled, w_proj):
    proj = jnp.dot(pooled, w_proj, preferred_element_type=jnp.float32)
    rnorm = lax.rsqrt(lax.optimization_barrier(jnp.sum(proj * proj, axis=-1, keepdims=True)) + 1e-06)
    return (proj * rnorm, rnorm)

def reference(tokens, seg_ids, counts, positives, w_qkv, w_out, ln_gain, w_proj):
    ranks = tokens.reshape(N_DP, TOK_DEV, D)

    def one_rank(pair):
        hidden = attend(pair[0], pair[1], w_qkv, w_out, ln_gain)
        return pool_rows(hidden, pair[1], SEG_DEV)
    pooled = lax.map(one_rank, (ranks, seg_ids)).reshape(NKEYS, D)
    unit, rnorm = embed_rows(pooled, w_proj)
    emb = unit.astype(jnp.bfloat16)
    logits = logit_scale * jnp.dot(emb, emb.T, preferred_element_type=jnp.float32)
    slot_ids = jnp.arange(NKEYS, dtype=jnp.int32)
    live = slot_ids % SEG_DEV < jnp.repeat(counts, SEG_DEV).astype(jnp.int32)
    allowed = live[None, :] & (slot_ids[None, :] != slot_ids[:, None])
    exp_logits = jnp.where(allowed, jnp.exp(logits), 0.0)
    denominator = lax.optimization_barrier(jnp.sum(exp_logits, axis=-1))
    target = slot_ids[None, :] == positives[:, None]
    picked = lax.optimization_barrier(jnp.sum(jnp.where(target, logits, 0.0), axis=-1))
    loss = jnp.where(live, jnp.log(denominator) - picked, 0.0)
    weights = jnp.where(live[:, None], exp_logits / denominator[:, None] - target.astype(jnp.float32), 0.0)
    weights = weights.astype(jnp.bfloat16)
    d_emb = logit_scale * (jnp.dot(weights, emb, preferred_element_type=jnp.float32) + jnp.dot(weights.T, emb, preferred_element_type=jnp.float32))
    radial = lax.optimization_barrier(jnp.sum(d_emb * unit, axis=-1, keepdims=True))
    d_proj = ((d_emb - radial * unit) * rnorm).astype(jnp.bfloat16)
    grad_pooled = jnp.dot(d_proj, w_proj.T, preferred_element_type=jnp.float32)
    return (loss, grad_pooled)
```

```python
import functools

import jax
import jax.numpy as jnp
from jax import lax
from jax.experimental import pallas as pl
from jax.experimental.pallas import tpu as pltpu
from jax.sharding import PartitionSpec as P

HEADS = 8
SCALE = 20.0
FAR = -1e30
MESH = pl.DeviceIdType.MESH
F32 = jnp.float32
BF16 = jnp.bfloat16
I32 = jnp.int32
NT = (((1,), (1,)), ((), ()))


def iota(shape, dim):
    return lax.broadcasted_iota(I32, shape, dim)


def attend_kernel(slots, seg_ref, tok_ref, wqkv_ref, wout_ref, gain_ref, pooled_ref, q_s, kt_s, v_s, qm_s, ctx_s, sum_s):
    rows, width = tok_ref.shape
    inner = wout_ref.shape[0]
    head_dim = inner // HEADS
    pairs = HEADS // 2
    tile = min(256, rows)
    qtile = 128
    seg = seg_ref[...]

    sub = iota((128, rows), 0)
    slot = sub % head_dim
    far = jnp.where(slot < slots, jnp.where(slot == seg, 0.0, FAR), 0.0)
    qm_s[...] = far.T.astype(BF16)
    half = iota((head_dim, rows), 0)
    onehot = jnp.where(half == seg, 1.0, 0.0).astype(BF16)
    for p in range(pairs):
        kt_s[2 * p, head_dim:, :] = onehot
        kt_s[2 * p + 1, :head_dim, :] = onehot

    def project(t, _):
        at = pl.ds(pl.multiple_of(t * tile, tile), tile)
        low = iota((tile, 128), 1) < head_dim
        x = tok_ref[at, :]
        qkv = jnp.dot(x, wqkv_ref[...], preferred_element_type=F32)
        q_s[at, :] = (qkv[:, :inner].astype(BF16) * head_dim**-0.5).astype(BF16)
        for p in range(pairs):
            k = qkv[:, inner + p * 128 : inner + (p + 1) * 128]
            kt = k.T.astype(BF16)
            kt_s[2 * p, :head_dim, at] = kt[:head_dim]
            kt_s[2 * p + 1, head_dim:, at] = kt[head_dim:]
            v = qkv[:, 2 * inner + p * 128 : 2 * inner + (p + 1) * 128]
            v_s[2 * p, at, :] = jnp.where(low, v, 1.0).astype(BF16)
            v_s[2 * p + 1, at, :] = jnp.where(low, 1.0, v).astype(BF16)
        return 0

    lax.fori_loop(0, rows // tile, project, 0)

    starts = [0] + [jnp.sum((seg < s).astype(F32)).astype(I32) for s in range(1, slots)] + [rows]

    def window(at, q0, first, span):
        keys = pl.ds(first, span)
        low = iota((qtile, 128), 1) < head_dim
        qm = qm_s[at, :]
        for p in range(pairs):
            q = q_s[at, p * 128 : (p + 1) * 128]
            out = []
            for h in range(2):
                qh = jnp.where(low, q, qm) if h == 0 else jnp.where(low, qm, q)
                s = jnp.dot(qh, kt_s[2 * p + h, :, keys], preferred_element_type=F32)
                e = jnp.exp(s - jnp.max(s, axis=1, keepdims=True)).astype(BF16)
                out.append(jnp.dot(e, v_s[2 * p + h, keys, :], preferred_element_type=F32))
            top = jnp.where(low, out[0], out[1])
            den = pltpu.roll(jnp.where(low, out[1], out[0]), head_dim, 1)
            ctx_s[at, p * 128 : (p + 1) * 128] = (top / den).astype(BF16)

    def queries(t, _):
        q0 = t * qtile
        at = pl.ds(pl.multiple_of(q0, qtile), qtile)
        lo = jnp.int32(0)
        hi = jnp.int32(rows)
        for s in range(1, slots):
            lo = jnp.where(starts[s] <= q0, starts[s], lo)
        for s in range(slots - 1, 0, -1):
            hi = jnp.where(starts[s] >= q0 + qtile, starts[s], hi)
        lo = lo // 128 * 128
        spans = [w for w in (512, 768) if w < rows] + [rows]
        below = jnp.int32(0)
        for w in spans:
            fits = hi - lo <= w

            @pl.when(fits & (below == 0))
            def _(w=w):
                first = 0 if w == rows else pl.multiple_of(jnp.minimum(lo, rows - w), 128)
                window(at, q0, first, w)

            below = jnp.where(fits, 1, below)
        return 0

    lax.fori_loop(0, rows // qtile, queries, 0)

    sum_s[...] = jnp.zeros_like(sum_s)

    def finish(t, _):
        at = pl.ds(pl.multiple_of(t * tile, tile), tile)
        resid = tok_ref[at, :].astype(F32) + jnp.dot(ctx_s[at, :], wout_ref[...], preferred_element_type=F32)
        centre = resid - jnp.sum(resid, axis=1, keepdims=True) * (1.0 / width)
        variance = jnp.sum(centre * centre, axis=1, keepdims=True) * (1.0 / width)
        hidden = (centre * lax.rsqrt(variance + 1e-05) * gain_ref[...]).astype(BF16)
        member = (iota((16, tile), 0) == seg_ref[:, at]).astype(F32).astype(BF16)
        sum_s[...] += jnp.dot(member, hidden, preferred_element_type=F32)
        return 0

    lax.fori_loop(0, rows // tile, finish, 0)
    sizes = jnp.sum((iota((16, rows), 0) == seg).astype(F32), axis=1, keepdims=True)
    pooled_ref[...] = (sum_s[:slots, :] / sizes[:slots]).astype(BF16)


def attend(seg, tokens, w_qkv, w_out, gain, slots):
    rows, width = tokens.shape
    inner = w_out.shape[0]
    vmem = pl.BlockSpec(memory_space=pltpu.VMEM)
    return pl.pallas_call(
        functools.partial(attend_kernel, slots),
        name="attend",
        out_shape=jax.ShapeDtypeStruct((slots, width), BF16),
        in_specs=[vmem] * 5,
        out_specs=vmem,
        scratch_shapes=[
            pltpu.VMEM((rows, inner), BF16),
            pltpu.VMEM((HEADS, 128, rows), BF16),
            pltpu.VMEM((HEADS, rows, 128), BF16),
            pltpu.VMEM((rows, 128), BF16),
            pltpu.VMEM((rows, inner), BF16),
            pltpu.VMEM((16, width), F32),
        ],
        compiler_params=pltpu.CompilerParams(vmem_limit_bytes=48 * 2**20),
    )(seg, tokens, w_qkv, w_out, gain)


def halves(x):
    hi = x.astype(BF16)
    return hi, (x - hi.astype(F32)).astype(BF16)


def loss_kernel(
    n_a, n_b, slots,
    counts_ref, pos_ref, pooled_ref, w_ref, loss_ref, grad_ref,
    colp, colm, rowg, drow, dcol, yrecv, ysend, mcol, mrow, mdr, mdc,
    p_j, g_i, unit_s, stack,
    s_colp, r_colp, s_colm, r_colm, s_row, r_row, s_dr, r_dr, s_dc, r_dc, s_y, r_y,
):
    me = lax.axis_index("dp")
    core, b, z = me % 2, (me // 2) % n_b, me // (2 * n_b)
    a = z * 2 + core
    width = pooled_ref.shape[1]
    r_rows = slots * n_b
    c_cols = slots * n_a

    def row_peer(k):
        o = (b + k) % n_b
        return o, z * (2 * n_b) + o * 2 + core

    def col_peer(k):
        o = (a + k) % n_a
        return o, (o // 2) * (2 * n_b) + b * 2 + o % 2

    barrier = pltpu.get_barrier_semaphore()

    def greet(peer):
        def step(k, _):
            pl.semaphore_signal(barrier, inc=1, device_id=(peer(k)[1],), device_id_type=MESH)
            return 0

        return step

    lax.fori_loop(1, n_b, greet(row_peer), 0)
    lax.fori_loop(1, n_a, greet(col_peer), 0)

    def exchange(peer, n, mine, source, dest, send, recv):
        def copy(k):
            o, device = peer(k)
            return pltpu.make_async_remote_copy(
                src_ref=source(o), dst_ref=dest.at[mine], send_sem=send.at[k], recv_sem=recv.at[mine],
                device_id=(device,), device_id_type=MESH,
            )

        def start():
            def step(k, _):
                copy(k).start()
                return 0

            lax.fori_loop(1, n, step, 0)

        def arrive():
            def step(k, _):
                o, device = peer(k)
                pltpu.make_async_remote_copy(
                    src_ref=source(o), dst_ref=dest.at[o], send_sem=send.at[k], recv_sem=recv.at[o],
                    device_id=(device,), device_id_type=MESH,
                ).wait_recv()
                return 0

            lax.fori_loop(1, n, step, 0)

        def drain():
            def step(k, _):
                copy(k).wait_send()
                return 0

            lax.fori_loop(1, n, step, 0)

        return start, arrive, drain

    x_colp = exchange(col_peer, n_a, a, lambda o: pooled_ref, colp, s_colp, r_colp)
    x_colm = exchange(col_peer, n_a, a, lambda o: mcol, colm, s_colm, r_colm)
    x_row = exchange(row_peer, n_b, b, lambda o: mrow, rowg, s_row, r_row)
    x_dr = exchange(row_peer, n_b, b, lambda o: mdr, drow, s_dr, r_dr)
    x_dc = exchange(col_peer, n_a, a, lambda o: mdc, dcol, s_dc, r_dc)
    x_y = exchange(row_peer, n_b, b, lambda o: ysend.at[o], yrecv, s_y, r_y)

    pl.semaphore_wait(barrier, n_a + n_b - 2)
    x_colp[0]()

    proj = jnp.dot(pooled_ref[...], w_ref[...], preferred_element_type=F32)
    rnorm = lax.rsqrt(jnp.sum(proj * proj, axis=1, keepdims=True) + 1e-06)
    unit = proj * rnorm
    unit_s[...] = unit
    s_row_id = iota((slots, 1), 0)
    mine_count = counts_ref[me]
    live_own = (s_row_id < mine_count).astype(F32)
    pos_own = jnp.zeros((slots, 1), F32)
    for s in range(slots):
        pos_own = jnp.where(s_row_id == s, pos_ref[s].astype(F32), pos_own)
    lane = iota((slots, 128), 1)
    here = lane == a * slots + iota((slots, 128), 0)
    mcol[...] = jnp.zeros_like(mcol)
    for r, value in enumerate((rnorm, pos_own, live_own)):
        mcol[r : r + 1, :] = jnp.sum(jnp.where(here, value, 0.0), axis=0, keepdims=True)
    x_colm[0]()
    g = SCALE * lax.dot_general(unit.astype(BF16), w_ref[...], NT, preferred_element_type=F32)
    mrow[:, :width] = g
    mrow[:, width:] = jnp.where(lane == 0, pos_own, jnp.where(lane == 1, live_own, 0.0))
    x_row[0]()

    colp[a] = pooled_ref[...]
    colm[a] = mcol[...]
    rowg[b] = mrow[...]
    p_j[...] = jnp.zeros_like(p_j)
    x_colp[1]()
    for o in range(n_a):
        p_j[o * slots : (o + 1) * slots, :] = colp[o].astype(F32)
    x_colm[1]()
    side = jnp.sum(colm[...], axis=0)
    rnorm_j, pos_j, live_j = side[0:1], side[1:2], side[2:3] > 0.5
    x_row[1]()
    for o in range(n_b):
        g_i[o * slots : (o + 1) * slots, :] = rowg[o]

    p_b = p_j[...].astype(BF16)
    g_hi, g_lo = halves(g_i[:, :width])
    tail = g_i[:, width:]
    pos_i, live_i = tail[:, 0:1], tail[:, 1:2] > 0.5
    logits = lax.dot_general(g_hi, p_b, NT, preferred_element_type=F32)
    logits += lax.dot_general(g_lo, p_b, NT, preferred_element_type=F32)
    logits = logits * rnorm_j
    r = iota((r_rows, 128), 0)
    c = iota((r_rows, 128), 1)
    id_i = (z * (2 * n_b) + (r // slots) * 2 + core) * slots + r % slots
    o_j = c // slots
    id_j = ((o_j // 2) * (2 * n_b) + b * 2 + o_j % 2) * slots + c % slots
    eye = r == c
    inside = (c < c_cols) & (id_i != id_j)
    expd = jnp.exp(jnp.where(c < c_cols, logits, 0.0))
    exp_i = jnp.where(inside & live_j, expd, 0.0)
    exp_j = jnp.where(inside & live_i, expd, 0.0)
    hit_i = (pos_i == id_j.astype(F32)) & (c < c_cols)
    hit_j = (pos_j == id_i.astype(F32)) & (c < c_cols)
    part_i = jnp.sum(exp_i, axis=1, keepdims=True)
    picked = jnp.sum(jnp.where(hit_i, logits, 0.0), axis=1, keepdims=True)
    mdr[...] = jnp.zeros_like(mdr)
    mdr[0:1, :] = jnp.sum(jnp.where(eye, part_i, 0.0), axis=0, keepdims=True)
    mdr[1:2, :] = jnp.sum(jnp.where(eye, picked, 0.0), axis=0, keepdims=True)
    mdc[...] = jnp.zeros_like(mdc)
    mdc[0:1, :] = jnp.sum(exp_j, axis=0, keepdims=True)
    x_dr[0]()
    x_dc[0]()
    drow[b] = mdr[...]
    dcol[a] = mdc[...]
    x_dr[1]()
    x_dc[1]()
    side_i = jnp.sum(drow[...], axis=0)
    den_j = jnp.sum(dcol[...], axis=0)[0:1]
    den_i = jnp.sum(jnp.where(eye, side_i[0:1], 0.0), axis=1, keepdims=True)
    w_i = jnp.where(live_i, exp_i / den_i - hit_i.astype(F32), 0.0).astype(BF16).astype(F32)
    den_j = jnp.where(den_j > 0.0, den_j, 1.0)
    w_j = jnp.where(live_j & (c < c_cols), exp_j / den_j - hit_j.astype(F32), 0.0).astype(BF16).astype(F32)
    mix_hi, mix_lo = halves((w_i + w_j) * rnorm_j)
    y = jnp.dot(mix_hi, p_b, preferred_element_type=F32) + jnp.dot(mix_lo, p_b, preferred_element_type=F32)
    for o in range(n_b):
        ysend[o] = y[o * slots : (o + 1) * slots]
    x_y[0]()
    yrecv[b] = ysend[b]

    table = jnp.log(side_i[0:1]) - side_i[1:2]
    mine = jnp.sum(jnp.where(lane == b * slots + iota((slots, 128), 0), table, 0.0), axis=1, keepdims=True)
    mine = jnp.where(live_own > 0.5, mine, 0.0)
    loss_lane = jnp.sum(jnp.where(lane == iota((slots, 128), 0), mine, 0.0), axis=0, keepdims=True)
    loss_ref[...] = loss_lane[:, :slots]

    x_y[1]()
    y_own = jnp.sum(yrecv[...], axis=0)
    y_hi = y_own.astype(BF16).astype(F32)
    stack[:slots, :] = y_hi
    stack[slots:, :] = y_own - y_hi
    d = jnp.dot(stack[...].astype(BF16), w_ref[...], preferred_element_type=F32)
    d_emb = SCALE * (d[:slots] + d[slots:])
    own = unit_s[...]
    radial = jnp.sum(d_emb * own, axis=1, keepdims=True)
    d_proj = ((d_emb - radial * own) * rnorm).astype(BF16)
    grad_ref[...] = lax.dot_general(d_proj, w_ref[...], NT, preferred_element_type=F32)
    for x in (x_colp, x_colm, x_row, x_dr, x_dc, x_y):
        x[2]()


def contrast(counts, positives, pooled, w_proj, n_a, n_b):
    slots, width = pooled.shape
    embed = w_proj.shape[1]
    vmem = pl.BlockSpec(memory_space=pltpu.VMEM)
    smem = pl.BlockSpec(memory_space=pltpu.SMEM)
    sems = [pltpu.SemaphoreType.DMA((n,)) for n in (n_a, n_a, n_a, n_a, n_b, n_b, n_b, n_b, n_a, n_a, n_b, n_b)]
    return pl.pallas_call(
        functools.partial(loss_kernel, n_a, n_b, slots),
        name="contrast",
        out_shape=(jax.ShapeDtypeStruct((1, slots), F32), jax.ShapeDtypeStruct((slots, width), F32)),
        in_specs=[smem, smem, vmem, vmem],
        out_specs=(vmem, vmem),
        scratch_shapes=[
            pltpu.VMEM((n_a, slots, width), BF16),
            pltpu.VMEM((n_a, 8, 128), F32),
            pltpu.VMEM((n_b, slots, width + 128), F32),
            pltpu.VMEM((n_b, 8, 128), F32),
            pltpu.VMEM((n_a, 8, 128), F32),
            pltpu.VMEM((n_b, slots, width), F32),
            pltpu.VMEM((n_b, slots, width), F32),
            pltpu.VMEM((8, 128), F32),
            pltpu.VMEM((slots, width + 128), F32),
            pltpu.VMEM((8, 128), F32),
            pltpu.VMEM((8, 128), F32),
            pltpu.VMEM((128, width), F32),
            pltpu.VMEM((slots * n_b, width + 128), F32),
            pltpu.VMEM((slots, embed), F32),
            pltpu.VMEM((2 * slots, width), F32),
            *sems,
        ],
        compiler_params=pltpu.CompilerParams(collective_id=0, has_side_effects=True, vmem_limit_bytes=32 * 2**20),
    )(counts, positives, pooled, w_proj)


def body(n_a, n_b, tokens, seg_ids, counts, positives, w_qkv, w_out, ln_gain, w_proj):
    slots = positives.shape[0]
    pooled = attend(seg_ids, tokens, w_qkv, w_out, ln_gain[None, :], slots)
    loss, grad = contrast(counts, positives, pooled, w_proj, n_a, n_b)
    return loss.reshape(slots), grad


def solution(mesh):
    n_b = 16
    n_a = mesh.size // n_b
    return jax.shard_map(
        functools.partial(body, n_a, n_b),
        mesh=mesh,
        in_specs=(P("dp", None), P("dp", None), P(), P("dp"), P(), P(), P(), P()),
        out_specs=(P("dp"), P("dp", None)),
        check_vma=False,
    )
```

```python
import functools

import jax
import jax.numpy as jnp
from jax import lax
from jax.experimental import pallas as pl
from jax.experimental.pallas import tpu as pltpu
from jax.sharding import PartitionSpec as P

HEADS = 8
SCALE = 20.0
FAR = -1e30
MESH = pl.DeviceIdType.MESH
F32 = jnp.float32
BF16 = jnp.bfloat16
I32 = jnp.int32
NT = (((1,), (1,)), ((), ()))


def iota(shape, dim):
    return lax.broadcasted_iota(I32, shape, dim)


def attend_kernel(slots, seg_ref, tok_hbm, wqkv_hbm, ctx_ref, tok_ref, wqkv_ref, q_s, kt_s, v_s, qm_s, sem):
    rows = tok_ref.shape[0]
    inner = ctx_ref.shape[1]
    head_dim = inner // HEADS
    pairs = HEADS // 2
    tile = min(256, rows)
    qtile = 128

    w_copy = pltpu.make_async_copy(wqkv_hbm, wqkv_ref, sem.at[0])
    w_copy.start()

    def tok_copy(t):
        at = pl.ds(pl.multiple_of(t * tile, tile), tile)
        return pltpu.make_async_copy(tok_hbm.at[at, :], tok_ref.at[at, :], sem.at[t + 1])

    for t in range(rows // tile):
        tok_copy(t).start()
    seg = seg_ref[...]

    sub = iota((128, rows), 0)
    slot = sub % head_dim
    far = jnp.where(slot < slots, jnp.where(slot == seg, 0.0, FAR), 0.0)
    qm_s[...] = far.T.astype(BF16)
    half = iota((head_dim, rows), 0)
    onehot = jnp.where(half == seg, 1.0, 0.0).astype(BF16)
    for p in range(pairs):
        kt_s[2 * p, head_dim:, :] = onehot
        kt_s[2 * p + 1, :head_dim, :] = onehot

    starts = [0] + [jnp.sum((seg < s).astype(F32)).astype(I32) for s in range(1, slots)] + [rows]

    w_copy.wait()

    def project(t, _):
        tok_copy(t).wait()
        at = pl.ds(pl.multiple_of(t * tile, tile), tile)
        low = iota((tile, 128), 1) < head_dim
        x = tok_ref[at, :]
        qkv = jnp.dot(x, wqkv_ref[...], preferred_element_type=F32)
        q_s[at, :] = (qkv[:, :inner].astype(BF16) * head_dim**-0.5).astype(BF16)
        for p in range(pairs):
            k = qkv[:, inner + p * 128 : inner + (p + 1) * 128]
            kt = k.T.astype(BF16)
            kt_s[2 * p, :head_dim, at] = kt[:head_dim]
            kt_s[2 * p + 1, head_dim:, at] = kt[head_dim:]
            v = qkv[:, 2 * inner + p * 128 : 2 * inner + (p + 1) * 128]
            v_s[2 * p, at, :] = jnp.where(low, v, 1.0).astype(BF16)
            v_s[2 * p + 1, at, :] = jnp.where(low, 1.0, v).astype(BF16)
        return 0

    lax.fori_loop(0, rows // tile, project, 0)

    def window(at, first, span):
        keys = pl.ds(first, span)
        low = iota((qtile, 128), 1) < head_dim
        qm = qm_s[at, :]
        scores = []
        for n in range(HEADS):
            q = q_s[at, n // 2 * 128 : (n // 2 + 1) * 128]
            q = jnp.where(low, q, qm) if n % 2 == 0 else jnp.where(low, qm, q)
            scores.append(jnp.dot(q, kt_s[n, :, keys], preferred_element_type=F32))
        exps = [jnp.exp(s - jnp.max(s, axis=1, keepdims=True)).astype(BF16) for s in scores]
        outs = [jnp.dot(e, v_s[n, keys, :], preferred_element_type=F32) for n, e in enumerate(exps)]
        for p in range(pairs):
            top = jnp.where(low, outs[2 * p], outs[2 * p + 1])
            den = pltpu.roll(jnp.where(low, outs[2 * p + 1], outs[2 * p]), head_dim, 1)
            ctx_ref[at, p * 128 : (p + 1) * 128] = (top / den).astype(BF16)

    def queries(t, _):
        q0 = t * qtile
        at = pl.ds(pl.multiple_of(q0, qtile), qtile)
        lo = jnp.int32(0)
        hi = jnp.int32(rows)
        for s in range(1, slots):
            lo = jnp.where(starts[s] <= q0, starts[s], lo)
        for s in range(slots - 1, 0, -1):
            hi = jnp.where(starts[s] >= q0 + qtile, starts[s], hi)
        lo = lo // 128 * 128
        spans = [w for w in (512, 768) if w < rows] + [rows]
        below = jnp.int32(0)
        for w in spans:
            fits = hi - lo <= w

            @pl.when(fits & (below == 0))
            def _(w=w):
                first = 0 if w == rows else pl.multiple_of(jnp.minimum(lo, rows - w), 128)
                window(at, first, w)

            below = jnp.where(fits, 1, below)
        return 0

    lax.fori_loop(0, rows // qtile, queries, 0)


def attend(seg, tokens, w_qkv, slots):
    rows, width = tokens.shape
    inner = w_qkv.shape[1] // 3
    vmem = pl.BlockSpec(memory_space=pltpu.VMEM)
    hbm = pl.BlockSpec(memory_space=pltpu.HBM)
    return pl.pallas_call(
        functools.partial(attend_kernel, slots),
        name="attend",
        out_shape=jax.ShapeDtypeStruct((rows, inner), BF16),
        in_specs=[vmem, hbm, hbm],
        out_specs=vmem,
        scratch_shapes=[
            pltpu.VMEM((rows, width), BF16),
            pltpu.VMEM((width, 3 * inner), BF16),
            pltpu.VMEM((rows, inner), BF16),
            pltpu.VMEM((HEADS, 128, rows), BF16),
            pltpu.VMEM((HEADS, rows, 128), BF16),
            pltpu.VMEM((rows, 128), BF16),
            pltpu.SemaphoreType.DMA((1 + rows // min(256, rows),)),
        ],
        compiler_params=pltpu.CompilerParams(vmem_limit_bytes=40 * 2**20),
        cost_estimate=pl.CostEstimate(flops=8 * 10**9, bytes_accessed=6 * 2**20, transcendentals=4 * 10**6),
    )(seg, tokens, w_qkv)


def halves(x):
    hi = x.astype(BF16)
    return hi, (x - hi.astype(F32)).astype(BF16)


def loss_kernel(
    n_a, n_b, slots,
    counts_ref, pos_ref, seg_ref, tok_ref, ctx_ref, wout_ref, gain_ref, w_ref, loss_ref, grad_ref,
    mine_s, colp, rowp, colm, rowm, drow, dcol, yrecv, ysend, mcol, mrow, mdr, mdc,
    sum_s, p_s, unit_s, emb_s, wt_s, stack,
    s_colp, r_colp, s_rowp, r_rowp, s_colm, r_colm, s_rowm, r_rowm, s_dr, r_dr, s_dc, r_dc, s_y, r_y,
):
    me = lax.axis_index("dp")
    core, b, z = me % 2, (me // 2) % n_b, me // (2 * n_b)
    a = z * 2 + core
    rows, width = tok_ref.shape
    embed = w_ref.shape[1]
    r_rows = slots * n_b
    c_cols = slots * n_a

    def row_peer(k):
        o = (b + k) % n_b
        return o, z * (2 * n_b) + o * 2 + core

    def col_peer(k):
        o = (a + k) % n_a
        return o, (o // 2) * (2 * n_b) + b * 2 + o % 2

    barrier = pltpu.get_barrier_semaphore()

    def greet(peer):
        def step(k, _):
            pl.semaphore_signal(barrier, inc=1, device_id=(peer(k)[1],), device_id_type=MESH)
            return 0

        return step

    lax.fori_loop(1, n_b, greet(row_peer), 0)
    lax.fori_loop(1, n_a, greet(col_peer), 0)

    def exchange(peer, n, mine, source, dest, send, recv):
        def copy(k):
            o, device = peer(k)
            return pltpu.make_async_remote_copy(
                src_ref=source(o), dst_ref=dest.at[mine], send_sem=send.at[k], recv_sem=recv.at[mine],
                device_id=(device,), device_id_type=MESH,
            )

        def start():
            def step(k, _):
                copy(k).start()
                return 0

            lax.fori_loop(1, n, step, 0)

        def arrive():
            def step(k, _):
                o, device = peer(k)
                pltpu.make_async_remote_copy(
                    src_ref=source(o), dst_ref=dest.at[o], send_sem=send.at[k], recv_sem=recv.at[o],
                    device_id=(device,), device_id_type=MESH,
                ).wait_recv()
                return 0

            lax.fori_loop(1, n, step, 0)

        def drain():
            def step(k, _):
                copy(k).wait_send()
                return 0

            lax.fori_loop(1, n, step, 0)

        return start, arrive, drain

    x_colp = exchange(col_peer, n_a, a, lambda o: mine_s, colp, s_colp, r_colp)
    x_rowp = exchange(row_peer, n_b, b, lambda o: mine_s, rowp, s_rowp, r_rowp)
    x_colm = exchange(col_peer, n_a, a, lambda o: mcol, colm, s_colm, r_colm)
    x_rowm = exchange(row_peer, n_b, b, lambda o: mrow, rowm, s_rowm, r_rowm)
    x_dr = exchange(row_peer, n_b, b, lambda o: mdr, drow, s_dr, r_dr)
    x_dc = exchange(col_peer, n_a, a, lambda o: mdc, dcol, s_dc, r_dc)
    x_y = exchange(row_peer, n_b, b, lambda o: ysend.at[o], yrecv, s_y, r_y)

    s_id = iota((slots, 1), 0)
    lane = iota((slots, 128), 1)
    live_own = (s_id < counts_ref[me]).astype(F32)
    pos_own = jnp.zeros((slots, 1), F32)
    for s in range(slots):
        pos_own = jnp.where(s_id == s, pos_ref[s].astype(F32), pos_own)
    for ref, first in ((mcol, a * slots), (mrow, b * slots)):
        here = lane == first + iota((slots, 128), 0)
        ref[0:1, :] = jnp.sum(jnp.where(here, pos_own, 0.0), axis=0, keepdims=True)
        ref[1:2, :] = jnp.sum(jnp.where(here, live_own, 0.0), axis=0, keepdims=True)

    tile = min(256, rows)
    sum_s[...] = jnp.zeros_like(sum_s)

    def finish(t, _):
        at = pl.ds(pl.multiple_of(t * tile, tile), tile)
        resid = tok_ref[at, :].astype(F32) + jnp.dot(ctx_ref[at, :], wout_ref[...], preferred_element_type=F32)
        centre = resid - jnp.sum(resid, axis=1, keepdims=True) * (1.0 / width)
        variance = jnp.sum(centre * centre, axis=1, keepdims=True) * (1.0 / width)
        hidden = (centre * lax.rsqrt(variance + 1e-05) * gain_ref[...]).astype(BF16)
        member = (iota((16, tile), 0) == seg_ref[:, at]).astype(F32).astype(BF16)
        sum_s[...] += jnp.dot(member, hidden, preferred_element_type=F32)
        return 0

    lax.fori_loop(0, rows // tile, finish, 0)
    sizes = jnp.sum((iota((16, rows), 0) == seg_ref[...]).astype(F32), axis=1, keepdims=True)
    pooled = (sum_s[:slots, :] / sizes[:slots]).astype(BF16)
    mine_s[...] = pooled

    pl.semaphore_wait(barrier, n_a + n_b - 2)
    x_colm[0]()
    x_rowm[0]()
    x_colp[0]()
    x_rowp[0]()

    proj = jnp.dot(pooled, w_ref[...], preferred_element_type=F32)
    rnorm = lax.rsqrt(jnp.sum(proj * proj, axis=1, keepdims=True) + 1e-06)
    unit_s[...] = proj * rnorm

    def turn(j, _):
        at = pl.ds(pl.multiple_of(j * 128, 128), 128)
        wt_s[at, :] = w_ref[:, at].T
        return 0

    lax.fori_loop(0, embed // 128, turn, 0)
    colp[a] = pooled
    rowp[b] = pooled
    colm[a] = mcol[...]
    rowm[b] = mrow[...]
    p_s[...] = jnp.zeros_like(p_s)
    x_colm[1]()
    x_rowm[1]()
    x_colp[1]()
    for o in range(n_a):
        p_s[o * slots : (o + 1) * slots, :] = colp[o].astype(F32)
    x_rowp[1]()
    for o in range(n_b):
        p_s[128 + o * slots : 128 + (o + 1) * slots, :] = rowp[o].astype(F32)

    p_b = p_s[...].astype(BF16)
    proj_all = jnp.dot(p_b, w_ref[...], preferred_element_type=F32)
    rnorm_all = lax.rsqrt(jnp.sum(proj_all * proj_all, axis=1, keepdims=True) + 1e-06)
    emb_s[...] = (proj_all * rnorm_all).astype(BF16)
    logits = SCALE * lax.dot_general(emb_s[128 : 128 + r_rows, :], emb_s[:128, :], NT, preferred_element_type=F32)

    r = iota((r_rows, 128), 0)
    c = iota((r_rows, 128), 1)
    id_i = (z * (2 * n_b) + (r // slots) * 2 + core) * slots + r % slots
    o_j = c // slots
    id_j = ((o_j // 2) * (2 * n_b) + b * 2 + o_j % 2) * slots + c % slots
    eye = r == c
    square = iota((128, 128), 0) == iota((128, 128), 1)
    rnorm_j = jnp.sum(jnp.where(square, rnorm_all[:128], 0.0), axis=0, keepdims=True)
    side_j = jnp.sum(colm[...], axis=0)
    side_i = jnp.sum(rowm[...], axis=0)
    pos_j, live_j = side_j[0:1], side_j[1:2] > 0.5
    pos_i = jnp.sum(jnp.where(eye, side_i[0:1], 0.0), axis=1, keepdims=True)
    live_i = jnp.sum(jnp.where(eye, side_i[1:2], 0.0), axis=1, keepdims=True) > 0.5
    inside = (c < c_cols) & (id_i != id_j)
    expd = jnp.exp(logits)
    exp_i = jnp.where(inside & live_j, expd, 0.0)
    exp_j = jnp.where(inside & live_i, expd, 0.0)
    hit_i = (pos_i == id_j.astype(F32)) & (c < c_cols)
    hit_j = (pos_j == id_i.astype(F32)) & (c < c_cols)
    part_i = jnp.sum(exp_i, axis=1, keepdims=True)
    picked = jnp.sum(jnp.where(hit_i, logits, 0.0), axis=1, keepdims=True)
    mdc[...] = jnp.sum(exp_j, axis=0, keepdims=True)
    mdr[0:1, :] = jnp.sum(jnp.where(eye, part_i, 0.0), axis=0, keepdims=True)
    mdr[1:2, :] = jnp.sum(jnp.where(eye, picked, 0.0), axis=0, keepdims=True)
    x_dc[0]()
    x_dr[0]()
    drow[b] = mdr[...]
    dcol[a] = mdc[...]
    x_dr[1]()
    x_dc[1]()
    sums_i = jnp.sum(drow[...], axis=0)
    den_j = jnp.sum(dcol[...], axis=0)
    den_i = jnp.sum(jnp.where(eye, sums_i[0:1], 0.0), axis=1, keepdims=True)
    w_i = jnp.where(live_i, exp_i / den_i - hit_i.astype(F32), 0.0)
    den_j = jnp.where(den_j > 0.0, den_j, 1.0)
    w_j = jnp.where(live_j & (c < c_cols), exp_j / den_j - hit_j.astype(F32), 0.0)
    mix_hi, mix_lo = halves((w_i + w_j) * rnorm_j)
    p_j = p_b[:128]
    y = jnp.dot(mix_hi, p_j, preferred_element_type=F32) + jnp.dot(mix_lo, p_j, preferred_element_type=F32)
    for o in range(n_b):
        ysend[o] = y[o * slots : (o + 1) * slots]
    x_y[0]()
    yrecv[b] = ysend[b]

    table = jnp.log(sums_i[0:1]) - sums_i[1:2]
    mine = jnp.sum(jnp.where(lane == b * slots + iota((slots, 128), 0), table, 0.0), axis=1, keepdims=True)
    mine = jnp.where(live_own > 0.5, mine, 0.0)
    loss_lane = jnp.sum(jnp.where(lane == iota((slots, 128), 0), mine, 0.0), axis=0, keepdims=True)
    loss_ref[...] = loss_lane[:, :slots]

    x_y[1]()
    y_own = jnp.sum(yrecv[...], axis=0)
    y_hi = y_own.astype(BF16).astype(F32)
    stack[:slots, :] = y_hi
    stack[slots:, :] = y_own - y_hi
    d = jnp.dot(stack[...].astype(BF16), w_ref[...], preferred_element_type=F32)
    d_emb = SCALE * (d[:slots] + d[slots:])
    own = unit_s[...]
    radial = jnp.sum(d_emb * own, axis=1, keepdims=True)
    d_proj = ((d_emb - radial * own) * rnorm).astype(BF16)
    grad_ref[...] = jnp.dot(d_proj, wt_s[...], preferred_element_type=F32)
    for x in (x_colm, x_rowm, x_colp, x_rowp, x_dr, x_dc, x_y):
        x[2]()


def contrast(counts, positives, seg, tokens, ctx, w_out, gain, w_proj, n_a, n_b):
    slots = positives.shape[0]
    width, embed = w_proj.shape
    vmem = pl.BlockSpec(memory_space=pltpu.VMEM)
    smem = pl.BlockSpec(memory_space=pltpu.SMEM)
    sems = [pltpu.SemaphoreType.DMA((n,)) for n in (n_a, n_b, n_a, n_b, n_b, n_a, n_b) for _ in range(2)]
    return pl.pallas_call(
        functools.partial(loss_kernel, n_a, n_b, slots),
        name="contrast",
        out_shape=(jax.ShapeDtypeStruct((1, slots), F32), jax.ShapeDtypeStruct((slots, width), F32)),
        in_specs=[smem, smem] + [vmem] * 6,
        out_specs=(vmem, vmem),
        scratch_shapes=[
            pltpu.VMEM((slots, width), BF16),
            pltpu.VMEM((n_a, slots, width), BF16),
            pltpu.VMEM((n_b, slots, width), BF16),
            pltpu.VMEM((n_a, 2, 128), F32),
            pltpu.VMEM((n_b, 2, 128), F32),
            pltpu.VMEM((n_b, 2, 128), F32),
            pltpu.VMEM((n_a, 1, 128), F32),
            pltpu.VMEM((n_b, slots, width), F32),
            pltpu.VMEM((n_b, slots, width), F32),
            pltpu.VMEM((2, 128), F32),
            pltpu.VMEM((2, 128), F32),
            pltpu.VMEM((2, 128), F32),
            pltpu.VMEM((1, 128), F32),
            pltpu.VMEM((16, width), F32),
            pltpu.VMEM((128 + slots * n_b, width), F32),
            pltpu.VMEM((slots, embed), F32),
            pltpu.VMEM((128 + slots * n_b, embed), BF16),
            pltpu.VMEM((embed, width), BF16),
            pltpu.VMEM((2 * slots, width), F32),
            *sems,
        ],
        compiler_params=pltpu.CompilerParams(collective_id=0, has_side_effects=True, vmem_limit_bytes=40 * 2**20),
    )(counts, positives, seg, tokens, ctx, w_out, gain, w_proj)


def body(n_a, n_b, tokens, seg_ids, counts, positives, w_qkv, w_out, ln_gain, w_proj):
    slots = positives.shape[0]
    ctx = attend(seg_ids, tokens, w_qkv, slots)
    loss, grad = contrast(counts, positives, seg_ids, tokens, ctx, w_out, ln_gain[None, :], w_proj, n_a, n_b)
    return loss.reshape(slots), grad


def solution(mesh):
    n_b = 16
    n_a = mesh.size // n_b
    return jax.shard_map(
        functools.partial(body, n_a, n_b),
        mesh=mesh,
        in_specs=(P("dp", None), P("dp", None), P(), P("dp"), P(), P(), P(), P()),
        out_specs=(P("dp"), P("dp", None)),
        check_vma=False,
    )
```

```python
import functools

import jax
import jax.numpy as jnp
from jax import lax
from jax.experimental import pallas as pl
from jax.experimental.pallas import tpu as pltpu
from jax.sharding import PartitionSpec as P

HEADS = 8
SCALE = 20.0
FAR = -1e30
MESH = pl.DeviceIdType.MESH
F32 = jnp.float32
BF16 = jnp.bfloat16
I32 = jnp.int32
NT = (((1,), (1,)), ((), ()))


def iota(shape, dim):
    return lax.broadcasted_iota(I32, shape, dim)


def attend_kernel(slots, seg_ref, tok_hbm, wqkv_hbm, ctx_ref, tok_ref, wqkv_ref, q_s, kt_s, v_s, qm_s, sem):
    rows = tok_ref.shape[0]
    inner = ctx_ref.shape[1]
    head_dim = inner // HEADS
    pairs = HEADS // 2
    tile = min(256, rows)
    qtile = 128

    w_copy = pltpu.make_async_copy(wqkv_hbm, wqkv_ref, sem.at[0])
    w_copy.start()

    def tok_copy(t):
        at = pl.ds(pl.multiple_of(t * tile, tile), tile)
        return pltpu.make_async_copy(tok_hbm.at[at, :], tok_ref.at[at, :], sem.at[t + 1])

    for t in range(rows // tile):
        tok_copy(t).start()
    seg = seg_ref[...]

    sub = iota((128, rows), 0)
    slot = sub % head_dim
    far = jnp.where(slot < slots, jnp.where(slot == seg, 0.0, FAR), 0.0)
    qm_s[...] = far.T.astype(BF16)
    half = iota((head_dim, rows), 0)
    onehot = jnp.where(half == seg, 1.0, 0.0).astype(BF16)
    for p in range(pairs):
        kt_s[2 * p, head_dim:, :] = onehot
        kt_s[2 * p + 1, :head_dim, :] = onehot

    starts = [0] + [jnp.sum((seg < s).astype(F32)).astype(I32) for s in range(1, slots)] + [rows]

    w_copy.wait()

    def project(t, _):
        tok_copy(t).wait()
        at = pl.ds(pl.multiple_of(t * tile, tile), tile)
        low = iota((tile, 128), 1) < head_dim
        x = tok_ref[at, :]
        qkv = jnp.dot(x, wqkv_ref[...], preferred_element_type=F32)
        q_s[at, :] = (qkv[:, :inner].astype(BF16) * head_dim**-0.5).astype(BF16)
        for p in range(pairs):
            k = qkv[:, inner + p * 128 : inner + (p + 1) * 128]
            kt = k.T.astype(BF16)
            kt_s[2 * p, :head_dim, at] = kt[:head_dim]
            kt_s[2 * p + 1, head_dim:, at] = kt[head_dim:]
            v = qkv[:, 2 * inner + p * 128 : 2 * inner + (p + 1) * 128]
            v_s[2 * p, at, :] = jnp.where(low, v, 1.0).astype(BF16)
            v_s[2 * p + 1, at, :] = jnp.where(low, 1.0, v).astype(BF16)
        return 0

    lax.fori_loop(0, rows // tile, project, 0)

    def window(at, first, span):
        keys = pl.ds(first, span)
        low = iota((qtile, 128), 1) < head_dim
        qm = qm_s[at, :]
        scores = []
        for n in range(HEADS):
            q = q_s[at, n // 2 * 128 : (n // 2 + 1) * 128]
            q = jnp.where(low, q, qm) if n % 2 == 0 else jnp.where(low, qm, q)
            scores.append(jnp.dot(q, kt_s[n, :, keys], preferred_element_type=F32))
        exps = [jnp.exp(s - jnp.max(s, axis=1, keepdims=True)).astype(BF16) for s in scores]
        outs = [jnp.dot(e, v_s[n, keys, :], preferred_element_type=F32) for n, e in enumerate(exps)]
        for p in range(pairs):
            top = jnp.where(low, outs[2 * p], outs[2 * p + 1])
            den = pltpu.roll(jnp.where(low, outs[2 * p + 1], outs[2 * p]), head_dim, 1)
            ctx_ref[at, p * 128 : (p + 1) * 128] = (top / den).astype(BF16)

    def queries(t, _):
        q0 = t * qtile
        at = pl.ds(pl.multiple_of(q0, qtile), qtile)
        lo = jnp.int32(0)
        hi = jnp.int32(rows)
        for s in range(1, slots):
            lo = jnp.where(starts[s] <= q0, starts[s], lo)
        for s in range(slots - 1, 0, -1):
            hi = jnp.where(starts[s] >= q0 + qtile, starts[s], hi)
        lo = lo // 128 * 128
        spans = [w for w in (512, 768) if w < rows] + [rows]
        below = jnp.int32(0)
        for w in spans:
            fits = hi - lo <= w

            @pl.when(fits & (below == 0))
            def _(w=w):
                first = 0 if w == rows else pl.multiple_of(jnp.minimum(lo, rows - w), 128)
                window(at, first, w)

            below = jnp.where(fits, 1, below)
        return 0

    lax.fori_loop(0, rows // qtile, queries, 0)


def attend(seg, tokens, w_qkv, slots):
    rows, width = tokens.shape
    inner = w_qkv.shape[1] // 3
    vmem = pl.BlockSpec(memory_space=pltpu.VMEM)
    hbm = pl.BlockSpec(memory_space=pltpu.HBM)
    return pl.pallas_call(
        functools.partial(attend_kernel, slots),
        name="attend",
        out_shape=jax.ShapeDtypeStruct((rows, inner), BF16),
        in_specs=[vmem, hbm, hbm],
        out_specs=vmem,
        scratch_shapes=[
            pltpu.VMEM((rows, width), BF16),
            pltpu.VMEM((width, 3 * inner), BF16),
            pltpu.VMEM((rows, inner), BF16),
            pltpu.VMEM((HEADS, 128, rows), BF16),
            pltpu.VMEM((HEADS, rows, 128), BF16),
            pltpu.VMEM((rows, 128), BF16),
            pltpu.SemaphoreType.DMA((1 + rows // min(256, rows),)),
        ],
        compiler_params=pltpu.CompilerParams(vmem_limit_bytes=40 * 2**20),
        cost_estimate=pl.CostEstimate(flops=8 * 10**9, bytes_accessed=6 * 2**20, transcendentals=4 * 10**6),
    )(seg, tokens, w_qkv)


def halves(x):
    hi = x.astype(BF16)
    return hi, (x - hi.astype(F32)).astype(BF16)


def loss_kernel(
    n_z, n_y, n_x, slots,
    counts_ref, pos_ref, seg_ref, tok_ref, ctx_ref, wout_ref, gain_ref, w_ref, loss_ref, grad_ref,
    mine_s, colp, rowp, drow, dcol, yrecv, ysend, mdr, mdc,
    sum_s, p_s, unit_s, emb_s, wt_s,
    s_colp, r_colp, s_rowp, r_rowp, s_dr, r_dr, s_dc, r_dc, s_y, r_y,
):
    n_a, n_b = n_z * 2, n_y * n_x
    me = lax.axis_index("dp")
    core, b, z = me % 2, (me // 2) % n_b, me // (2 * n_b)
    a = z * 2 + core
    rows, width = tok_ref.shape
    embed = w_ref.shape[1]
    r_rows = slots * n_b
    c_cols = slots * n_a

    def ring(d, n):
        return min(d, n - d)

    row_peers = []
    for dy in range(n_y):
        for dx in range(n_x):
            o = (b // n_x + dy) % n_y * n_x + (b % n_x + dx) % n_x
            row_peers.append((2 * ring(dy, n_y) + 2 * ring(dx, n_x), o, z * (2 * n_b) + o * 2 + core))
    col_peers = []
    for dz in range(n_z):
        for dc in range(2):
            o = (z + dz) % n_z * 2 + (core + dc) % 2
            col_peers.append((2 * ring(dz, n_z) + dc, o, (o // 2) * (2 * n_b) + b * 2 + o % 2))
    row_peers, col_peers = row_peers[1:], col_peers[1:]

    barrier = pltpu.get_barrier_semaphore()
    for _, _, device in row_peers + col_peers:
        pl.semaphore_signal(barrier, inc=1, device_id=(device,), device_id_type=MESH)

    def exchange(peers, mine, source, dest, send, recv):
        out = []
        for k, (hops, o, device) in enumerate(peers):
            out.append((
                hops,
                functools.partial(
                    pltpu.make_async_remote_copy, src_ref=source(o), dst_ref=dest.at[mine], send_sem=send.at[k],
                    recv_sem=recv.at[mine], device_id=(device,), device_id_type=MESH,
                ),
                functools.partial(
                    pltpu.make_async_remote_copy, src_ref=source(o), dst_ref=dest.at[o], send_sem=send.at[k],
                    recv_sem=recv.at[o], device_id=(device,), device_id_type=MESH,
                ),
            ))
        return sorted(out, key=lambda c: -c[0])

    def start(*exchanges):
        for _, copy, _ in sorted(sum(exchanges, []), key=lambda c: -c[0]):
            copy().start()

    def arrive(exchange):
        for _, _, copy in reversed(exchange):
            copy().wait_recv()

    x_col = exchange(col_peers, a, lambda o: mine_s, colp, s_colp, r_colp)
    x_row = exchange(row_peers, b, lambda o: mine_s, rowp, s_rowp, r_rowp)
    x_dr = exchange(row_peers, b, lambda o: mdr, drow, s_dr, r_dr)
    x_dc = exchange(col_peers, a, lambda o: mdc, dcol, s_dc, r_dc)
    x_y = exchange(row_peers, b, lambda o: ysend.at[o], yrecv, s_y, r_y)

    s_id = iota((slots, 1), 0)
    lane = iota((slots, 128), 1)
    live_own = (s_id < counts_ref[me]).astype(F32)
    side = jnp.where(lane == 2, live_own, 0.0)
    for s in range(slots):
        own_row = iota((slots, 128), 0) == s
        side = jnp.where(own_row & (lane == 0), (pos_ref[s] // 32).astype(F32), side)
        side = jnp.where(own_row & (lane == 1), (pos_ref[s] % 32).astype(F32), side)
    mine_s[:, width:] = side.astype(BF16)

    tile = min(256, rows)
    sum_s[...] = jnp.zeros_like(sum_s)

    def finish(t, _):
        at = pl.ds(pl.multiple_of(t * tile, tile), tile)
        resid = tok_ref[at, :].astype(F32) + jnp.dot(ctx_ref[at, :], wout_ref[...], preferred_element_type=F32)
        centre = resid - jnp.sum(resid, axis=1, keepdims=True) * (1.0 / width)
        variance = jnp.sum(centre * centre, axis=1, keepdims=True) * (1.0 / width)
        hidden = (centre * lax.rsqrt(variance + 1e-05) * gain_ref[...]).astype(BF16)
        member = (iota((16, tile), 0) == seg_ref[:, at]).astype(F32).astype(BF16)
        sum_s[...] += jnp.dot(member, hidden, preferred_element_type=F32)
        return 0

    lax.fori_loop(0, rows // tile, finish, 0)
    sizes = jnp.sum((iota((16, rows), 0) == seg_ref[...]).astype(F32), axis=1, keepdims=True)
    pooled = (sum_s[:slots, :] / sizes[:slots]).astype(BF16)
    mine_s[:, :width] = pooled

    pl.semaphore_wait(barrier, n_a + n_b - 2)
    start(x_col, x_row)

    proj = jnp.dot(pooled, w_ref[...], preferred_element_type=F32)
    rnorm = lax.rsqrt(jnp.sum(proj * proj, axis=1, keepdims=True) + 1e-06)
    unit_s[...] = proj * rnorm

    def turn(j, _):
        at = pl.ds(pl.multiple_of(j * 128, 128), 128)
        wt_s[at, :] = w_ref[:, at].T
        return 0

    lax.fori_loop(0, embed // 128, turn, 0)
    colp[a] = mine_s[...]
    rowp[b] = mine_s[...]
    p_s[...] = jnp.zeros_like(p_s)
    arrive(x_row)
    for o in range(n_b):
        p_s[128 + o * slots : 128 + (o + 1) * slots, :] = rowp[o].astype(F32)
    arrive(x_col)
    for o in range(n_a):
        p_s[o * slots : (o + 1) * slots, :] = colp[o].astype(F32)

    proj_all = jnp.dot(p_s[:, :width].astype(BF16), w_ref[...], preferred_element_type=F32)
    rnorm_all = lax.rsqrt(jnp.sum(proj_all * proj_all, axis=1, keepdims=True) + 1e-06)
    emb_s[...] = (proj_all * rnorm_all).astype(BF16)
    emb_j = emb_s[:128, :]
    logits = SCALE * lax.dot_general(emb_s[128 : 128 + r_rows, :], emb_j, NT, preferred_element_type=F32)

    r = iota((r_rows, 128), 0)
    c = iota((r_rows, 128), 1)
    id_i = (z * (2 * n_b) + (r // slots) * 2 + core) * slots + r % slots
    o_j = c // slots
    id_j = ((o_j // 2) * (2 * n_b) + b * 2 + o_j % 2) * slots + c % slots
    eye = r == c
    square = iota((128, 128), 0) == iota((128, 128), 1)

    def along(column):
        return jnp.sum(jnp.where(square, column, 0.0), axis=0, keepdims=True)

    side_j = p_s[:128, width:]
    side_i = p_s[128 : 128 + r_rows, width:]
    pos_i, live_i = side_i[:, 0:1] * 32.0 + side_i[:, 1:2], side_i[:, 2:3] > 0.5
    pos_j, live_j = along(side_j[:, 0:1] * 32.0 + side_j[:, 1:2]), along(side_j[:, 2:3]) > 0.5
    inside = (c < c_cols) & (id_i != id_j)
    expd = jnp.exp(logits)
    exp_i = jnp.where(inside & live_j, expd, 0.0)
    exp_j = jnp.where(inside & live_i, expd, 0.0)
    hit_i = (pos_i == id_j.astype(F32)) & (c < c_cols)
    hit_j = (pos_j == id_i.astype(F32)) & (c < c_cols)
    part_i = jnp.sum(exp_i, axis=1, keepdims=True)
    picked = jnp.sum(jnp.where(hit_i, logits, 0.0), axis=1, keepdims=True)
    mdc[...] = jnp.sum(exp_j, axis=0, keepdims=True)
    mdr[0:1, :] = jnp.sum(jnp.where(eye, part_i, 0.0), axis=0, keepdims=True)
    mdr[1:2, :] = jnp.sum(jnp.where(eye, picked, 0.0), axis=0, keepdims=True)
    start(x_dr, x_dc)
    drow[b] = mdr[...]
    dcol[a] = mdc[...]
    arrive(x_dr)
    arrive(x_dc)
    sums_i = jnp.sum(drow[...], axis=0)
    den_j = jnp.sum(dcol[...], axis=0)
    den_i = jnp.sum(jnp.where(eye, sums_i[0:1], 0.0), axis=1, keepdims=True)
    w_i = jnp.where(live_i, exp_i / den_i - hit_i.astype(F32), 0.0)
    den_j = jnp.where(den_j > 0.0, den_j, 1.0)
    w_j = jnp.where(live_j & (c < c_cols), exp_j / den_j - hit_j.astype(F32), 0.0)
    mix = jnp.concatenate(halves(w_i + w_j), axis=0)
    y = jnp.dot(mix, emb_j, preferred_element_type=F32)
    y = (y[:r_rows] + y[r_rows:]).astype(BF16)
    for o in range(n_b):
        ysend[o] = y[o * slots : (o + 1) * slots]
    start(x_y)
    yrecv[b] = ysend[b]

    table = jnp.log(sums_i[0:1]) - sums_i[1:2]
    mine = jnp.sum(jnp.where(lane == b * slots + iota((slots, 128), 0), table, 0.0), axis=1, keepdims=True)
    mine = jnp.where(live_own > 0.5, mine, 0.0)
    loss_lane = jnp.sum(jnp.where(lane == iota((slots, 128), 0), mine, 0.0), axis=0, keepdims=True)
    loss_ref[...] = loss_lane[:, :slots]

    arrive(x_y)
    d_emb = SCALE * jnp.sum(yrecv[...].astype(F32), axis=0)
    own = unit_s[...]
    radial = jnp.sum(d_emb * own, axis=1, keepdims=True)
    d_proj = ((d_emb - radial * own) * rnorm).astype(BF16)
    grad_ref[...] = jnp.dot(d_proj, wt_s[...], preferred_element_type=F32)
    for x in (x_col, x_row, x_dr, x_dc, x_y):
        for _, copy, _ in x:
            copy().wait_send()


def contrast(counts, positives, seg, tokens, ctx, w_out, gain, w_proj, n_z, n_y, n_x):
    slots = positives.shape[0]
    n_a, n_b = n_z * 2, n_y * n_x
    width, embed = w_proj.shape
    vmem = pl.BlockSpec(memory_space=pltpu.VMEM)
    smem = pl.BlockSpec(memory_space=pltpu.SMEM)
    sems = [pltpu.SemaphoreType.DMA((n,)) for n in (n_a, n_b, n_b, n_a, n_b) for _ in range(2)]
    return pl.pallas_call(
        functools.partial(loss_kernel, n_z, n_y, n_x, slots),
        name="contrast",
        out_shape=(jax.ShapeDtypeStruct((1, slots), F32), jax.ShapeDtypeStruct((slots, width), F32)),
        in_specs=[smem, smem] + [vmem] * 6,
        out_specs=(vmem, vmem),
        scratch_shapes=[
            pltpu.VMEM((slots, width + 128), BF16),
            pltpu.VMEM((n_a, slots, width + 128), BF16),
            pltpu.VMEM((n_b, slots, width + 128), BF16),
            pltpu.VMEM((n_b, 2, 128), F32),
            pltpu.VMEM((n_a, 1, 128), F32),
            pltpu.VMEM((n_b, slots, embed), BF16),
            pltpu.VMEM((n_b, slots, embed), BF16),
            pltpu.VMEM((2, 128), F32),
            pltpu.VMEM((1, 128), F32),
            pltpu.VMEM((16, width), F32),
            pltpu.VMEM((128 + slots * n_b, width + 128), F32),
            pltpu.VMEM((slots, embed), F32),
            pltpu.VMEM((128 + slots * n_b, embed), BF16),
            pltpu.VMEM((embed, width), BF16),
            *sems,
        ],
        compiler_params=pltpu.CompilerParams(collective_id=0, has_side_effects=True, vmem_limit_bytes=40 * 2**20),
    )(counts, positives, seg, tokens, ctx, w_out, gain, w_proj)


def body(grid, tokens, seg_ids, counts, positives, w_qkv, w_out, ln_gain, w_proj):
    slots = positives.shape[0]
    in_hbm = functools.partial(pltpu.with_memory_space_constraint, memory_space=pltpu.HBM)
    ctx = attend(seg_ids, in_hbm(tokens), in_hbm(w_qkv), slots)
    loss, grad = contrast(counts, positives, seg_ids, tokens, ctx, w_out, ln_gain[None, :], w_proj, *grid)
    return loss.reshape(slots), grad


def solution(mesh):
    grid = (mesh.size // 32, 4, 4)
    return jax.shard_map(
        functools.partial(body, grid),
        mesh=mesh,
        in_specs=(P("dp", None), P("dp", None), P(), P("dp"), P(), P(), P(), P()),
        out_specs=(P("dp"), P("dp", None)),
        check_vma=False,
    )
```

```python
import functools

import jax
import jax.numpy as jnp
from jax import lax
from jax.experimental import pallas as pl
from jax.experimental.pallas import tpu as pltpu
from jax.sharding import PartitionSpec as P

HEADS = 8
SCALE = 20.0
FAR = -1e30
MESH = pl.DeviceIdType.MESH
F32 = jnp.float32
BF16 = jnp.bfloat16
I32 = jnp.int32
NT = (((1,), (1,)), ((), ()))


def iota(shape, dim):
    return lax.broadcasted_iota(I32, shape, dim)


def attend_kernel(
    slots, seg_hbm, tok_hbm, wqkv_hbm, wout_hbm, wproj_hbm, ctx_ref, tok_ref, wout_ref, wproj_ref, seg_ref, wqkv_ref, q_s, kt_s, v_s, qm_s, sem,
):
    rows = tok_ref.shape[0]
    inner = ctx_ref.shape[1]
    head_dim = inner // HEADS
    pairs = HEADS // 2
    tile = min(256, rows)
    qtile = 128

    seg_copy = pltpu.make_async_copy(seg_hbm, seg_ref, sem.at[1 + rows // tile])
    seg_copy.start()
    w_copy = pltpu.make_async_copy(wqkv_hbm, wqkv_ref, sem.at[0])
    w_copy.start()

    def tok_copy(t):
        at = pl.ds(pl.multiple_of(t * tile, tile), tile)
        return pltpu.make_async_copy(tok_hbm.at[at, :], tok_ref.at[at, :], sem.at[t + 1])

    for t in range(rows // tile):
        tok_copy(t).start()
    seg_copy.wait()
    seg = seg_ref[...]

    sub = iota((128, rows), 0)
    slot = sub % head_dim
    far = jnp.where(slot < slots, jnp.where(slot == seg, 0.0, FAR), 0.0)
    qm_s[...] = far.T.astype(BF16)
    half = iota((head_dim, rows), 0)
    onehot = jnp.where(half == seg, 1.0, 0.0).astype(BF16)
    for p in range(pairs):
        kt_s[2 * p, head_dim:, :] = onehot
        kt_s[2 * p + 1, :head_dim, :] = onehot

    starts = [0] + [jnp.sum((seg < s).astype(F32)).astype(I32) for s in range(1, slots)] + [rows]

    w_copy.wait()

    def project(t, _):
        tok_copy(t).wait()
        at = pl.ds(pl.multiple_of(t * tile, tile), tile)
        low = iota((tile, 128), 1) < head_dim
        x = tok_ref[at, :]
        qkv = jnp.dot(x, wqkv_ref[...], preferred_element_type=F32)
        q_s[at, :] = (qkv[:, :inner].astype(BF16) * head_dim**-0.5).astype(BF16)
        for p in range(pairs):
            k = qkv[:, inner + p * 128 : inner + (p + 1) * 128]
            kt = k.T.astype(BF16)
            kt_s[2 * p, :head_dim, at] = kt[:head_dim]
            kt_s[2 * p + 1, head_dim:, at] = kt[head_dim:]
            v = qkv[:, 2 * inner + p * 128 : 2 * inner + (p + 1) * 128]
            v_s[2 * p, at, :] = jnp.where(low, v, 1.0).astype(BF16)
            v_s[2 * p + 1, at, :] = jnp.where(low, 1.0, v).astype(BF16)
        return 0

    lax.fori_loop(0, rows // tile, project, 0)

    later = [
        pltpu.make_async_copy(wout_hbm, wout_ref, sem.at[2 + rows // tile]),
        pltpu.make_async_copy(wproj_hbm, wproj_ref, sem.at[3 + rows // tile]),
    ]
    for copy in later:
        copy.start()

    def window(tiles, span):
        low = iota((qtile, 128), 1) < head_dim
        scores = []
        for at, first in tiles:
            qm = qm_s[at, :]
            for n in range(HEADS):
                q = q_s[at, n // 2 * 128 : (n // 2 + 1) * 128]
                q = jnp.where(low, q, qm) if n % 2 == 0 else jnp.where(low, qm, q)
                scores.append(jnp.dot(q, kt_s[n, :, pl.ds(first, span)], preferred_element_type=F32))
        exps = [jnp.exp(s - jnp.max(s, axis=1, keepdims=True)).astype(BF16) for s in scores]
        outs = []
        for i, (at, first) in enumerate(tiles):
            for n in range(HEADS):
                outs.append(jnp.dot(exps[i * HEADS + n], v_s[n, pl.ds(first, span), :], preferred_element_type=F32))
        for i, (at, first) in enumerate(tiles):
            for p in range(pairs):
                even, odd = outs[i * HEADS + 2 * p], outs[i * HEADS + 2 * p + 1]
                top = jnp.where(low, even, odd)
                den = pltpu.roll(jnp.where(low, odd, even), head_dim, 1)
                ctx_ref[at, p * 128 : (p + 1) * 128] = (top / den).astype(BF16)

    group = min(2, rows // qtile)

    def queries(t, _):
        los, width_needed = [], jnp.int32(0)
        for i in range(group):
            q0 = (t * group + i) * qtile
            lo = jnp.int32(0)
            hi = jnp.int32(rows)
            for s in range(1, slots):
                lo = jnp.where(starts[s] <= q0, starts[s], lo)
            for s in range(slots - 1, 0, -1):
                hi = jnp.where(starts[s] >= q0 + qtile, starts[s], hi)
            lo = lo // 128 * 128
            los.append(lo)
            width_needed = jnp.maximum(width_needed, hi - lo)
        spans = [w for w in (384, 512, 640, 768) if w < rows] + [rows]
        for below, w in zip([0] + spans, spans):

            @pl.when((width_needed > below) & (width_needed <= w))
            def _(w=w):
                tiles = []
                for i in range(group):
                    at = pl.ds(pl.multiple_of((t * group + i) * qtile, qtile), qtile)
                    tiles.append((at, 0 if w == rows else pl.multiple_of(jnp.minimum(los[i], rows - w), 128)))
                window(tiles, w)

        return 0

    lax.fori_loop(0, rows // (qtile * group), queries, 0)
    for copy in later:
        copy.wait()


def attend(seg, tokens, w_qkv, w_out, w_proj, slots):
    rows, width = tokens.shape
    inner = w_qkv.shape[1] // 3
    vmem = pl.BlockSpec(memory_space=pltpu.VMEM)
    hbm = pl.BlockSpec(memory_space=pltpu.HBM)
    return pl.pallas_call(
        functools.partial(attend_kernel, slots),
        name="attend",
        out_shape=[jax.ShapeDtypeStruct(x, BF16) for x in ((rows, inner), tokens.shape, w_out.shape, w_proj.shape)],
        in_specs=[hbm] * 5,
        out_specs=[vmem] * 4,
        scratch_shapes=[
            pltpu.VMEM((1, rows), I32),
            pltpu.VMEM((width, 3 * inner), BF16),
            pltpu.VMEM((rows, inner), BF16),
            pltpu.VMEM((HEADS, 128, rows), BF16),
            pltpu.VMEM((HEADS, rows, 128), BF16),
            pltpu.VMEM((rows, 128), BF16),
            pltpu.SemaphoreType.DMA((4 + rows // min(256, rows),)),
        ],
        compiler_params=pltpu.CompilerParams(vmem_limit_bytes=40 * 2**20),
        cost_estimate=pl.CostEstimate(flops=8 * 10**9, bytes_accessed=6 * 2**20, transcendentals=4 * 10**6),
    )(seg, tokens, w_qkv, w_out, w_proj)


def halves(x):
    hi = x.astype(BF16)
    return hi, (x - hi.astype(F32)).astype(BF16)


def loss_kernel(
    n_z, n_y, n_x, slots,
    counts_ref, pos_ref, seg_ref, tok_ref, ctx_ref, wout_ref, gain_ref, w_ref, loss_ref, grad_ref,
    mine_s, colp, rowp, drow, dcol, yrecv, ysend, mdr, mdc,
    p_s, unit_s, emb_s, wt_s,
    s_colp, r_colp, s_rowp, r_rowp, s_dr, r_dr, s_dc, r_dc, s_y, r_y,
):
    n_a, n_b = n_z * 2, n_y * n_x
    me = lax.axis_index("dp")
    core, b, z = me % 2, (me // 2) % n_b, me // (2 * n_b)
    a = z * 2 + core
    rows, width = tok_ref.shape
    embed = w_ref.shape[1]
    r_rows = slots * n_b
    c_cols = slots * n_a

    def ring(d, n):
        return min(d, n - d)

    row_peers = []
    for dy in range(n_y):
        for dx in range(n_x):
            o = (b // n_x + dy) % n_y * n_x + (b % n_x + dx) % n_x
            row_peers.append((2 * ring(dy, n_y) + 2 * ring(dx, n_x), o, z * (2 * n_b) + o * 2 + core))
    col_peers = []
    for dz in range(n_z):
        for dc in range(2):
            o = (z + dz) % n_z * 2 + (core + dc) % 2
            col_peers.append((2 * ring(dz, n_z) + dc, o, (o // 2) * (2 * n_b) + b * 2 + o % 2))
    row_peers, col_peers = row_peers[1:], col_peers[1:]

    barrier = pltpu.get_barrier_semaphore()
    for _, _, device in row_peers + col_peers:
        pl.semaphore_signal(barrier, inc=1, device_id=(device,), device_id_type=MESH)

    def exchange(peers, mine, source, dest, send, recv):
        out = []
        for k, (hops, o, device) in enumerate(peers):
            out.append((
                hops,
                functools.partial(
                    pltpu.make_async_remote_copy, src_ref=source(o), dst_ref=dest.at[mine], send_sem=send.at[k],
                    recv_sem=recv.at[mine], device_id=(device,), device_id_type=MESH,
                ),
                functools.partial(
                    pltpu.make_async_remote_copy, src_ref=source(o), dst_ref=dest.at[o], send_sem=send.at[k],
                    recv_sem=recv.at[o], device_id=(device,), device_id_type=MESH,
                ),
            ))
        return sorted(out, key=lambda c: -c[0])

    def start(*exchanges):
        for _, copy, _ in sorted(sum(exchanges, []), key=lambda c: -c[0]):
            copy().start()

    def arrive(exchange):
        for _, _, copy in reversed(exchange):
            copy().wait_recv()

    x_col = exchange(col_peers, a, lambda o: mine_s, colp, s_colp, r_colp)
    x_row = exchange(row_peers, b, lambda o: mine_s, rowp, s_rowp, r_rowp)
    x_dr = exchange(row_peers, b, lambda o: mdr, drow, s_dr, r_dr)
    x_dc = exchange(col_peers, a, lambda o: mdc, dcol, s_dc, r_dc)
    x_y = exchange(row_peers, b, lambda o: ysend.at[o], yrecv, s_y, r_y)

    s_id = iota((slots, 1), 0)
    lane = iota((slots, 128), 1)
    n_devices = counts_ref.shape[1]
    my_count = jnp.sum(jnp.where(iota((1, n_devices), 1) == me, counts_ref[...], 0).astype(F32), axis=1, keepdims=True)
    live_own = (s_id.astype(F32) < my_count).astype(F32)
    diagonal = iota((slots, slots), 0) == iota((slots, slots), 1)

    def down(values):
        return jnp.sum(jnp.where(diagonal, values.astype(F32), 0.0), axis=1, keepdims=True)

    places = pos_ref[...]
    side = jnp.where(lane == 0, down(places >> 5), jnp.where(lane == 1, down(places & 31), 0.0))
    side = jnp.where(lane == 2, live_own, side)
    mine_s[:, width:] = side.astype(BF16)

    tile = min(256, rows)

    def mix_in(t):
        at = pl.ds(t * tile, tile)
        return tok_ref[at, :].astype(F32) + jnp.dot(ctx_ref[at, :], wout_ref[...], preferred_element_type=F32)

    def norm(resid):
        centre = resid - jnp.sum(resid, axis=1, keepdims=True) * (1.0 / width)
        variance = jnp.sum(centre * centre, axis=1, keepdims=True) * (1.0 / width)
        return (centre * lax.rsqrt(variance + 1e-05) * gain_ref[...]).astype(BF16)

    def pool(t, hidden):
        member = (iota((16, tile), 0) == seg_ref[:, pl.ds(t * tile, tile)]).astype(F32).astype(BF16)
        return jnp.dot(member, hidden, preferred_element_type=F32)

    resids = [mix_in(t) for t in range(rows // tile)]
    sums = sum(pool(t, norm(resid)) for t, resid in enumerate(resids))
    sizes = jnp.sum((iota((16, rows), 0) == seg_ref[...]).astype(F32), axis=1, keepdims=True)
    pooled = (sums[:slots] / sizes[:slots]).astype(BF16)
    mine_s[:, :width] = pooled

    pl.semaphore_wait(barrier, n_a + n_b - 2)
    start(x_col, x_row)

    proj = jnp.dot(pooled, w_ref[...], preferred_element_type=F32)
    rnorm = lax.rsqrt(jnp.sum(proj * proj, axis=1, keepdims=True) + 1e-06)
    unit_s[...] = proj * rnorm

    def turn(j, _):
        at = pl.ds(pl.multiple_of(j * 128, 128), 128)
        wt_s[at, :] = w_ref[:, at].T
        return 0

    lax.fori_loop(0, embed // 128, turn, 0)
    colp[a] = mine_s[...]
    rowp[b] = mine_s[...]
    p_s[...] = jnp.zeros_like(p_s)
    arrive(x_row)
    for o in range(n_b):
        p_s[128 + o * slots : 128 + (o + 1) * slots, :] = rowp[o].astype(F32)
    arrive(x_col)
    for o in range(n_a):
        p_s[o * slots : (o + 1) * slots, :] = colp[o].astype(F32)

    proj_all = jnp.dot(p_s[:, :width].astype(BF16), w_ref[...], preferred_element_type=F32)
    rnorm_all = lax.rsqrt(jnp.sum(proj_all * proj_all, axis=1, keepdims=True) + 1e-06)
    emb_s[...] = (proj_all * rnorm_all).astype(BF16)
    emb_j = emb_s[:128, :]
    logits = SCALE * lax.dot_general(emb_s[128 : 128 + r_rows, :], emb_j, NT, preferred_element_type=F32)

    r = iota((r_rows, 128), 0)
    c = iota((r_rows, 128), 1)
    id_i = (z * (2 * n_b) + (r // slots) * 2 + core) * slots + r % slots
    o_j = c // slots
    id_j = ((o_j // 2) * (2 * n_b) + b * 2 + o_j % 2) * slots + c % slots
    eye = r == c
    square = iota((128, 128), 0) == iota((128, 128), 1)

    def along(column):
        return jnp.sum(jnp.where(square, column, 0.0), axis=0, keepdims=True)

    side_j = p_s[:128, width:]
    side_i = p_s[128 : 128 + r_rows, width:]
    pos_i, live_i = side_i[:, 0:1] * 32.0 + side_i[:, 1:2], side_i[:, 2:3] > 0.5
    pos_j, live_j = along(side_j[:, 0:1] * 32.0 + side_j[:, 1:2]), along(side_j[:, 2:3]) > 0.5
    inside = (c < c_cols) & (id_i != id_j)
    expd = jnp.exp(logits)
    exp_i = jnp.where(inside & live_j, expd, 0.0)
    exp_j = jnp.where(inside & live_i, expd, 0.0)
    hit_i = (pos_i == id_j.astype(F32)) & (c < c_cols)
    hit_j = (pos_j == id_i.astype(F32)) & (c < c_cols)
    part_i = jnp.sum(exp_i, axis=1, keepdims=True)
    picked = jnp.sum(jnp.where(hit_i, logits, 0.0), axis=1, keepdims=True)
    mdc[...] = jnp.sum(exp_j, axis=0, keepdims=True)
    mdr[0:1, :] = jnp.sum(jnp.where(eye, part_i, 0.0), axis=0, keepdims=True)
    mdr[1:2, :] = jnp.sum(jnp.where(eye, picked, 0.0), axis=0, keepdims=True)
    start(x_dr, x_dc)
    drow[b] = mdr[...]
    dcol[a] = mdc[...]
    arrive(x_dr)
    arrive(x_dc)
    sums_i = jnp.sum(drow[...], axis=0)
    den_j = jnp.sum(dcol[...], axis=0)
    den_i = jnp.sum(jnp.where(eye, sums_i[0:1], 0.0), axis=1, keepdims=True)
    w_i = jnp.where(live_i, exp_i / den_i - hit_i.astype(F32), 0.0)
    den_j = jnp.where(den_j > 0.0, den_j, 1.0)
    w_j = jnp.where(live_j & (c < c_cols), exp_j / den_j - hit_j.astype(F32), 0.0)
    mix = jnp.concatenate(halves(w_i + w_j), axis=0)
    y = jnp.dot(mix, emb_j, preferred_element_type=F32)
    y = (y[:r_rows] + y[r_rows:]).astype(BF16)
    for o in range(n_b):
        ysend[o] = y[o * slots : (o + 1) * slots]
    start(x_y)
    yrecv[b] = ysend[b]

    table = jnp.log(sums_i[0:1]) - sums_i[1:2]
    mine = jnp.sum(jnp.where(lane == b * slots + iota((slots, 128), 0), table, 0.0), axis=1, keepdims=True)
    mine = jnp.where(live_own > 0.5, mine, 0.0)
    loss_lane = jnp.sum(jnp.where(lane == iota((slots, 128), 0), mine, 0.0), axis=0, keepdims=True)
    loss_ref[...] = loss_lane[:, :slots]

    arrive(x_y)
    d_emb = SCALE * jnp.sum(yrecv[...].astype(F32), axis=0)
    own = unit_s[...]
    radial = jnp.sum(d_emb * own, axis=1, keepdims=True)
    d_proj = ((d_emb - radial * own) * rnorm).astype(BF16)
    grad_ref[...] = jnp.dot(d_proj, wt_s[...], preferred_element_type=F32)
    for x in (x_col, x_row, x_dr, x_dc, x_y):
        for _, copy, _ in x:
            copy().wait_send()


def contrast(counts, positives, seg, tokens, ctx, w_out, gain, w_proj, n_z, n_y, n_x):
    slots = positives.shape[1]
    n_a, n_b = n_z * 2, n_y * n_x
    width, embed = w_proj.shape
    vmem = pl.BlockSpec(memory_space=pltpu.VMEM)
    sems = [pltpu.SemaphoreType.DMA((n,)) for n in (n_a, n_b, n_b, n_a, n_b) for _ in range(2)]
    return pl.pallas_call(
        functools.partial(loss_kernel, n_z, n_y, n_x, slots),
        name="contrast",
        out_shape=(jax.ShapeDtypeStruct((1, slots), F32), jax.ShapeDtypeStruct((slots, width), F32)),
        in_specs=[vmem] * 8,
        out_specs=(vmem, vmem),
        scratch_shapes=[
            pltpu.VMEM((slots, width + 128), BF16),
            pltpu.VMEM((n_a, slots, width + 128), BF16),
            pltpu.VMEM((n_b, slots, width + 128), BF16),
            pltpu.VMEM((n_b, 2, 128), F32),
            pltpu.VMEM((n_a, 1, 128), F32),
            pltpu.VMEM((n_b, slots, embed), BF16),
            pltpu.VMEM((n_b, slots, embed), BF16),
            pltpu.VMEM((2, 128), F32),
            pltpu.VMEM((1, 128), F32),
            pltpu.VMEM((128 + slots * n_b, width + 128), F32),
            pltpu.VMEM((slots, embed), F32),
            pltpu.VMEM((128 + slots * n_b, embed), BF16),
            pltpu.VMEM((embed, width), BF16),
            *sems,
        ],
        compiler_params=pltpu.CompilerParams(collective_id=0, has_side_effects=True, vmem_limit_bytes=40 * 2**20),
    )(counts, positives, seg, tokens, ctx, w_out, gain, w_proj)


def body(grid, tokens, seg_ids, counts, positives, w_qkv, w_out, ln_gain, w_proj):
    slots = positives.shape[0]
    in_hbm = functools.partial(pltpu.with_memory_space_constraint, memory_space=pltpu.HBM)
    ctx, tokens, w_out, w_proj = attend(*map(in_hbm, (seg_ids, tokens, w_qkv, w_out, w_proj)), slots)
    loss, grad = contrast(counts[None, :], positives[None, :], seg_ids, tokens, ctx, w_out, ln_gain[None, :], w_proj, *grid)
    return loss.reshape(slots), grad


def solution(mesh):
    grid = (mesh.size // 32, 4, 4)
    return jax.shard_map(
        functools.partial(body, grid),
        mesh=mesh,
        in_specs=(P("dp", None), P("dp", None), P(), P("dp"), P(), P(), P(), P()),
        out_specs=(P("dp"), P("dp", None)),
        check_vma=False,
    )
```

```python
import functools

import jax
import jax.numpy as jnp
from jax import lax
from jax.experimental import pallas as pl
from jax.experimental.pallas import tpu as pltpu
from jax.sharding import PartitionSpec as P

HEADS = 8
SCALE = 20.0
FAR = -1e30
MESH = pl.DeviceIdType.MESH
F32 = jnp.float32
BF16 = jnp.bfloat16
I32 = jnp.int32
NT = (((1,), (1,)), ((), ()))


def iota(shape, dim):
    return lax.broadcasted_iota(I32, shape, dim)


def attend_kernel(
    slots, seg_hbm, tok_hbm, wqkv_hbm, wout_hbm, wproj_hbm, ctx_ref, tok_ref, wout_ref, wproj_ref, seg_ref, wqkv_ref, q_s, kt_s, v_s, qm_s, sem,
):
    rows = tok_ref.shape[0]
    inner = ctx_ref.shape[1]
    head_dim = inner // HEADS
    pairs = HEADS // 2
    tile = min(256, rows)
    qtile = 128

    seg_copy = pltpu.make_async_copy(seg_hbm, seg_ref, sem.at[1 + rows // tile])
    seg_copy.start()
    w_copy = pltpu.make_async_copy(wqkv_hbm, wqkv_ref, sem.at[0])
    w_copy.start()

    def tok_copy(t):
        at = pl.ds(pl.multiple_of(t * tile, tile), tile)
        return pltpu.make_async_copy(tok_hbm.at[at, :], tok_ref.at[at, :], sem.at[t + 1])

    for t in range(rows // tile):
        tok_copy(t).start()
    seg_copy.wait()
    seg = seg_ref[...]

    sub = iota((128, rows), 0)
    slot = sub % head_dim
    far = jnp.where(slot < slots, jnp.where(slot == seg, 0.0, FAR), 0.0)
    qm_s[...] = far.T.astype(BF16)
    half = iota((head_dim, rows), 0)
    onehot = jnp.where(half == seg, 1.0, 0.0).astype(BF16)
    for p in range(pairs):
        kt_s[2 * p, head_dim:, :] = onehot
        kt_s[2 * p + 1, :head_dim, :] = onehot

    starts = [0] + [jnp.sum((seg < s).astype(F32)).astype(I32) for s in range(1, slots)] + [rows]

    w_copy.wait()

    def project(t, _):
        tok_copy(t).wait()
        at = pl.ds(pl.multiple_of(t * tile, tile), tile)
        low = iota((tile, 128), 1) < head_dim
        x = tok_ref[at, :]
        qkv = jnp.dot(x, wqkv_ref[...], preferred_element_type=F32)
        q_s[at, :] = (qkv[:, :inner].astype(BF16) * head_dim**-0.5).astype(BF16)
        for p in range(pairs):
            k = qkv[:, inner + p * 128 : inner + (p + 1) * 128]
            kt = k.T.astype(BF16)
            kt_s[2 * p, :head_dim, at] = kt[:head_dim]
            kt_s[2 * p + 1, head_dim:, at] = kt[head_dim:]
            v = qkv[:, 2 * inner + p * 128 : 2 * inner + (p + 1) * 128]
            v_s[2 * p, at, :] = jnp.where(low, v, 1.0).astype(BF16)
            v_s[2 * p + 1, at, :] = jnp.where(low, 1.0, v).astype(BF16)
        return 0

    lax.fori_loop(0, rows // tile, project, 0)

    later = [
        pltpu.make_async_copy(wout_hbm, wout_ref, sem.at[2 + rows // tile]),
        pltpu.make_async_copy(wproj_hbm, wproj_ref, sem.at[3 + rows // tile]),
    ]
    for copy in later:
        copy.start()

    def window(tiles, span):
        low = iota((qtile, 128), 1) < head_dim
        scores = []
        for at, first in tiles:
            qm = qm_s[at, :]
            for n in range(HEADS):
                q = q_s[at, n // 2 * 128 : (n // 2 + 1) * 128]
                q = jnp.where(low, q, qm) if n % 2 == 0 else jnp.where(low, qm, q)
                scores.append(jnp.dot(q, kt_s[n, :, pl.ds(first, span)], preferred_element_type=F32))
        exps = [jnp.exp(s - jnp.max(s, axis=1, keepdims=True)).astype(BF16) for s in scores]
        outs = []
        for i, (at, first) in enumerate(tiles):
            for n in range(HEADS):
                outs.append(jnp.dot(exps[i * HEADS + n], v_s[n, pl.ds(first, span), :], preferred_element_type=F32))
        for i, (at, first) in enumerate(tiles):
            for p in range(pairs):
                even, odd = outs[i * HEADS + 2 * p], outs[i * HEADS + 2 * p + 1]
                top = jnp.where(low, even, odd)
                den = pltpu.roll(jnp.where(low, odd, even), head_dim, 1)
                ctx_ref[at, p * 128 : (p + 1) * 128] = (top / den).astype(BF16)

    group = 1

    def queries(t, _):
        los, width_needed = [], jnp.int32(0)
        for i in range(group):
            q0 = (t * group + i) * qtile
            lo = jnp.int32(0)
            hi = jnp.int32(rows)
            for s in range(1, slots):
                lo = jnp.where(starts[s] <= q0, starts[s], lo)
            for s in range(slots - 1, 0, -1):
                hi = jnp.where(starts[s] >= q0 + qtile, starts[s], hi)
            lo = lo // 128 * 128
            los.append(lo)
            width_needed = jnp.maximum(width_needed, hi - lo)
        spans = [w for w in (256, 384, 512, 640, 768, 896) if w < rows] + [rows]
        for below, w in zip([0] + spans, spans):

            @pl.when((width_needed > below) & (width_needed <= w))
            def _(w=w):
                tiles = []
                for i in range(group):
                    at = pl.ds(pl.multiple_of((t * group + i) * qtile, qtile), qtile)
                    tiles.append((at, 0 if w == rows else pl.multiple_of(jnp.minimum(los[i], rows - w), 128)))
                window(tiles, w)

        return 0

    lax.fori_loop(0, rows // (qtile * group), queries, 0)
    for copy in later:
        copy.wait()


def attend(seg, tokens, w_qkv, w_out, w_proj, slots):
    rows, width = tokens.shape
    inner = w_qkv.shape[1] // 3
    vmem = pl.BlockSpec(memory_space=pltpu.VMEM)
    hbm = pl.BlockSpec(memory_space=pltpu.HBM)
    return pl.pallas_call(
        functools.partial(attend_kernel, slots),
        name="attend",
        out_shape=[jax.ShapeDtypeStruct(x, BF16) for x in ((rows, inner), tokens.shape, w_out.shape, w_proj.shape)],
        in_specs=[hbm] * 5,
        out_specs=[vmem] * 4,
        scratch_shapes=[
            pltpu.VMEM((1, rows), I32),
            pltpu.VMEM((width, 3 * inner), BF16),
            pltpu.VMEM((rows, inner), BF16),
            pltpu.VMEM((HEADS, 128, rows), BF16),
            pltpu.VMEM((HEADS, rows, 128), BF16),
            pltpu.VMEM((rows, 128), BF16),
            pltpu.SemaphoreType.DMA((4 + rows // min(256, rows),)),
        ],
        compiler_params=pltpu.CompilerParams(vmem_limit_bytes=40 * 2**20),
        cost_estimate=pl.CostEstimate(flops=8 * 10**9, bytes_accessed=6 * 2**20, transcendentals=4 * 10**6),
    )(seg, tokens, w_qkv, w_out, w_proj)


def halves(x):
    hi = x.astype(BF16)
    return hi, (x - hi.astype(F32)).astype(BF16)


def loss_kernel(
    n_z, n_y, n_x, slots,
    counts_ref, pos_ref, seg_ref, tok_ref, ctx_ref, wout_ref, gain_ref, w_ref, loss_ref, grad_ref,
    mine_s, colp, rowp, drow, dcol, yrecv, ysend, mdr, mdc,
    p_s, unit_s, emb_s, wt_s,
    s_colp, r_colp, s_rowp, r_rowp, s_dr, r_dr, s_dc, r_dc, s_y, r_y,
):
    n_a, n_b = n_z * 2, n_y * n_x
    me = lax.axis_index("dp")
    core, b, z = me % 2, (me // 2) % n_b, me // (2 * n_b)
    a = z * 2 + core
    rows, width = tok_ref.shape
    embed = w_ref.shape[1]
    r_rows = slots * n_b
    c_cols = slots * n_a

    def ring(d, n):
        return min(d, n - d)

    row_peers = []
    for dy in range(n_y):
        for dx in range(n_x):
            o = (b // n_x + dy) % n_y * n_x + (b % n_x + dx) % n_x
            row_peers.append((2 * ring(dy, n_y) + 2 * ring(dx, n_x), o, z * (2 * n_b) + o * 2 + core))
    col_peers = []
    for dz in range(n_z):
        for dc in range(2):
            o = (z + dz) % n_z * 2 + (core + dc) % 2
            col_peers.append((2 * ring(dz, n_z) + dc, o, (o // 2) * (2 * n_b) + b * 2 + o % 2))
    row_peers, col_peers = row_peers[1:], col_peers[1:]

    barrier = pltpu.get_barrier_semaphore()
    for _, _, device in row_peers + col_peers:
        pl.semaphore_signal(barrier, inc=1, device_id=(device,), device_id_type=MESH)

    def exchange(peers, mine, source, dest, send, recv):
        out = []
        for k, (hops, o, device) in enumerate(peers):
            out.append((
                hops,
                functools.partial(
                    pltpu.make_async_remote_copy, src_ref=source(o), dst_ref=dest.at[mine], send_sem=send.at[k],
                    recv_sem=recv.at[mine], device_id=(device,), device_id_type=MESH,
                ),
                functools.partial(
                    pltpu.make_async_remote_copy, src_ref=source(o), dst_ref=dest.at[o], send_sem=send.at[k],
                    recv_sem=recv.at[o], device_id=(device,), device_id_type=MESH,
                ),
            ))
        return sorted(out, key=lambda c: -c[0])

    def start(*exchanges):
        for _, copy, _ in sorted(sum(exchanges, []), key=lambda c: -c[0]):
            copy().start()

    def arrive(exchange):
        for _, _, copy in reversed(exchange):
            copy().wait_recv()

    x_col = exchange(col_peers, a, lambda o: mine_s, colp, s_colp, r_colp)
    x_row = exchange(row_peers, b, lambda o: mine_s, rowp, s_rowp, r_rowp)
    x_dr = exchange(row_peers, b, lambda o: mdr, drow, s_dr, r_dr)
    x_dc = exchange(col_peers, a, lambda o: mdc, dcol, s_dc, r_dc)
    x_y = exchange(row_peers, b, lambda o: ysend.at[o], yrecv, s_y, r_y)

    s_id = iota((slots, 1), 0)
    lane = iota((slots, 128), 1)
    n_devices = counts_ref.shape[1]
    my_count = jnp.sum(jnp.where(iota((1, n_devices), 1) == me, counts_ref[...], 0).astype(F32), axis=1, keepdims=True)
    live_own = (s_id.astype(F32) < my_count).astype(F32)
    diagonal = iota((slots, slots), 0) == iota((slots, slots), 1)

    def down(values):
        return jnp.sum(jnp.where(diagonal, values.astype(F32), 0.0), axis=1, keepdims=True)

    places = pos_ref[...]
    side = jnp.where(lane == 0, down(places >> 5), jnp.where(lane == 1, down(places & 31), 0.0))
    side = jnp.where(lane == 2, live_own, side)
    mine_s[:, width:] = side.astype(BF16)

    tile = min(256, rows)

    def mix_in(t):
        at = pl.ds(t * tile, tile)
        return tok_ref[at, :].astype(F32) + jnp.dot(ctx_ref[at, :], wout_ref[...], preferred_element_type=F32)

    def norm(resid):
        centre = resid - jnp.sum(resid, axis=1, keepdims=True) * (1.0 / width)
        variance = jnp.sum(centre * centre, axis=1, keepdims=True) * (1.0 / width)
        return (centre * lax.rsqrt(variance + 1e-05) * gain_ref[...]).astype(BF16)

    def pool(t, hidden):
        member = (iota((16, tile), 0) == seg_ref[:, pl.ds(t * tile, tile)]).astype(F32).astype(BF16)
        return jnp.dot(member, hidden, preferred_element_type=F32)

    resids = [mix_in(t) for t in range(rows // tile)]
    sums = sum(pool(t, norm(resid)) for t, resid in enumerate(resids))
    sizes = jnp.sum((iota((16, rows), 0) == seg_ref[...]).astype(F32), axis=1, keepdims=True)
    pooled = (sums[:slots] / sizes[:slots]).astype(BF16)
    mine_s[:, :width] = pooled

    pl.semaphore_wait(barrier, n_a + n_b - 2)
    start(x_col, x_row)

    proj = jnp.dot(pooled, w_ref[...], preferred_element_type=F32)
    rnorm = lax.rsqrt(jnp.sum(proj * proj, axis=1, keepdims=True) + 1e-06)
    unit_s[...] = proj * rnorm

    def turn(j, _):
        at = pl.ds(pl.multiple_of(j * 128, 128), 128)
        wt_s[at, :] = w_ref[:, at].T
        return 0

    lax.fori_loop(0, embed // 128, turn, 0)
    colp[a] = mine_s[...]
    rowp[b] = mine_s[...]
    p_s[...] = jnp.zeros_like(p_s)
    arrive(x_row)
    for o in range(n_b):
        p_s[128 + o * slots : 128 + (o + 1) * slots, :] = rowp[o].astype(F32)
    arrive(x_col)
    for o in range(n_a):
        p_s[o * slots : (o + 1) * slots, :] = colp[o].astype(F32)

    proj_all = jnp.dot(p_s[:, :width].astype(BF16), w_ref[...], preferred_element_type=F32)
    rnorm_all = lax.rsqrt(jnp.sum(proj_all * proj_all, axis=1, keepdims=True) + 1e-06)
    emb_s[...] = (proj_all * rnorm_all).astype(BF16)
    emb_j = emb_s[:128, :]
    logits = SCALE * lax.dot_general(emb_s[128 : 128 + r_rows, :], emb_j, NT, preferred_element_type=F32)

    r = iota((r_rows, 128), 0)
    c = iota((r_rows, 128), 1)
    id_i = (z * (2 * n_b) + (r // slots) * 2 + core) * slots + r % slots
    o_j = c // slots
    id_j = ((o_j // 2) * (2 * n_b) + b * 2 + o_j % 2) * slots + c % slots
    eye = r == c
    square = iota((128, 128), 0) == iota((128, 128), 1)

    def along(column):
        return jnp.sum(jnp.where(square, column, 0.0), axis=0, keepdims=True)

    side_j = p_s[:128, width:]
    side_i = p_s[128 : 128 + r_rows, width:]
    pos_i, live_i = side_i[:, 0:1] * 32.0 + side_i[:, 1:2], side_i[:, 2:3] > 0.5
    pos_j, live_j = along(side_j[:, 0:1] * 32.0 + side_j[:, 1:2]), along(side_j[:, 2:3]) > 0.5
    inside = (c < c_cols) & (id_i != id_j)
    expd = jnp.exp(logits)
    exp_i = jnp.where(inside & live_j, expd, 0.0)
    exp_j = jnp.where(inside & live_i, expd, 0.0)
    hit_i = (pos_i == id_j.astype(F32)) & (c < c_cols)
    hit_j = (pos_j == id_i.astype(F32)) & (c < c_cols)
    part_i = jnp.sum(exp_i, axis=1, keepdims=True)
    picked = jnp.sum(jnp.where(hit_i, logits, 0.0), axis=1, keepdims=True)
    mdc[...] = jnp.sum(exp_j, axis=0, keepdims=True)
    mdr[0:1, :] = jnp.sum(jnp.where(eye, part_i, 0.0), axis=0, keepdims=True)
    mdr[1:2, :] = jnp.sum(jnp.where(eye, picked, 0.0), axis=0, keepdims=True)
    start(x_dr, x_dc)
    drow[b] = mdr[...]
    dcol[a] = mdc[...]
    arrive(x_dr)
    arrive(x_dc)
    sums_i = jnp.sum(drow[...], axis=0)
    den_j = jnp.sum(dcol[...], axis=0)
    den_i = jnp.sum(jnp.where(eye, sums_i[0:1], 0.0), axis=1, keepdims=True)
    w_i = jnp.where(live_i, exp_i / den_i - hit_i.astype(F32), 0.0)
    den_j = jnp.where(den_j > 0.0, den_j, 1.0)
    w_j = jnp.where(live_j & (c < c_cols), exp_j / den_j - hit_j.astype(F32), 0.0)
    mix = jnp.concatenate(halves(w_i + w_j), axis=0)
    y = jnp.dot(mix, emb_j, preferred_element_type=F32)
    y = (y[:r_rows] + y[r_rows:]).astype(BF16)
    for o in range(n_b):
        ysend[o] = y[o * slots : (o + 1) * slots]
    start(x_y)
    yrecv[b] = ysend[b]

    table = jnp.log(sums_i[0:1]) - sums_i[1:2]
    mine = jnp.sum(jnp.where(lane == b * slots + iota((slots, 128), 0), table, 0.0), axis=1, keepdims=True)
    mine = jnp.where(live_own > 0.5, mine, 0.0)
    loss_lane = jnp.sum(jnp.where(lane == iota((slots, 128), 0), mine, 0.0), axis=0, keepdims=True)
    loss_ref[...] = loss_lane[:, :slots]

    arrive(x_y)
    d_emb = SCALE * jnp.sum(yrecv[...].astype(F32), axis=0)
    own = unit_s[...]
    radial = jnp.sum(d_emb * own, axis=1, keepdims=True)
    d_proj = ((d_emb - radial * own) * rnorm).astype(BF16)
    grad_ref[...] = jnp.dot(d_proj, wt_s[...], preferred_element_type=F32)
    for x in (x_col, x_row, x_dr, x_dc, x_y):
        for _, copy, _ in x:
            copy().wait_send()


def contrast(counts, positives, seg, tokens, ctx, w_out, gain, w_proj, n_z, n_y, n_x):
    slots = positives.shape[1]
    n_a, n_b = n_z * 2, n_y * n_x
    width, embed = w_proj.shape
    vmem = pl.BlockSpec(memory_space=pltpu.VMEM)
    sems = [pltpu.SemaphoreType.DMA((n,)) for n in (n_a, n_b, n_b, n_a, n_b) for _ in range(2)]
    return pl.pallas_call(
        functools.partial(loss_kernel, n_z, n_y, n_x, slots),
        name="contrast",
        out_shape=(jax.ShapeDtypeStruct((1, slots), F32), jax.ShapeDtypeStruct((slots, width), F32)),
        in_specs=[vmem] * 8,
        out_specs=(vmem, vmem),
        scratch_shapes=[
            pltpu.VMEM((slots, width + 128), BF16),
            pltpu.VMEM((n_a, slots, width + 128), BF16),
            pltpu.VMEM((n_b, slots, width + 128), BF16),
            pltpu.VMEM((n_b, 2, 128), F32),
            pltpu.VMEM((n_a, 1, 128), F32),
            pltpu.VMEM((n_b, slots, embed), BF16),
            pltpu.VMEM((n_b, slots, embed), BF16),
            pltpu.VMEM((2, 128), F32),
            pltpu.VMEM((1, 128), F32),
            pltpu.VMEM((128 + slots * n_b, width + 128), F32),
            pltpu.VMEM((slots, embed), F32),
            pltpu.VMEM((128 + slots * n_b, embed), BF16),
            pltpu.VMEM((embed, width), BF16),
            *sems,
        ],
        compiler_params=pltpu.CompilerParams(collective_id=0, has_side_effects=True, vmem_limit_bytes=40 * 2**20),
    )(counts, positives, seg, tokens, ctx, w_out, gain, w_proj)


def deliver_kernel(loss_ref, grad_ref, loss_hbm, grad_hbm, sem):
    copies = [pltpu.make_async_copy(loss_ref, loss_hbm, sem.at[0]), pltpu.make_async_copy(grad_ref, grad_hbm, sem.at[1])]
    for copy in copies:
        copy.start()
    for copy in copies:
        copy.wait()


def deliver(loss, grad):
    vmem = pl.BlockSpec(memory_space=pltpu.VMEM)
    hbm = pl.BlockSpec(memory_space=pltpu.HBM)
    return pl.pallas_call(
        deliver_kernel,
        name="deliver",
        out_shape=(jax.ShapeDtypeStruct(loss.shape, F32), jax.ShapeDtypeStruct(grad.shape, F32)),
        in_specs=[vmem, vmem],
        out_specs=(hbm, hbm),
        scratch_shapes=[pltpu.SemaphoreType.DMA((2,))],
        compiler_params=pltpu.CompilerParams(vmem_limit_bytes=2**20),
    )(loss, grad)


def body(grid, tokens, seg_ids, counts, positives, w_qkv, w_out, ln_gain, w_proj):
    slots = positives.shape[0]
    in_hbm = functools.partial(pltpu.with_memory_space_constraint, memory_space=pltpu.HBM)
    ctx, tokens, w_out, w_proj = attend(*map(in_hbm, (seg_ids, tokens, w_qkv, w_out, w_proj)), slots)
    loss, grad = contrast(counts[None, :], positives[None, :], seg_ids, tokens, ctx, w_out, ln_gain[None, :], w_proj, *grid)
    loss, grad = deliver(loss, grad)
    return loss.reshape(slots), grad


def solution(mesh):
    grid = (mesh.size // 32, 4, 4)
    return jax.shard_map(
        functools.partial(body, grid),
        mesh=mesh,
        in_specs=(P("dp", None), P("dp", None), P(), P("dp"), P(), P(), P(), P()),
        out_specs=(P("dp"), P("dp", None)),
        check_vma=False,
    )
```

```python
import functools

import jax
import jax.numpy as jnp
from jax import lax
from jax.experimental import pallas as pl
from jax.experimental.pallas import tpu as pltpu
from jax.sharding import PartitionSpec as P

HEADS = 8
SCALE = 20.0
TILE = 128
FAR = -1e30
MESH = pl.DeviceIdType.MESH
F32 = jnp.float32
BF16 = jnp.bfloat16
I32 = jnp.int32
NT = (((1,), (1,)), ((), ()))


def iota(shape, dim):
    return lax.broadcasted_iota(I32, shape, dim)


def context(queries, far, kt_ref, v_ref, keys):
    pairs = HEADS // 2
    low = iota((TILE, 128), 1) < 64
    scores = []
    for n in range(HEADS):
        q = queries[:, n // 2 * 128 : (n // 2 + 1) * 128]
        q = jnp.where(low, q, far) if n % 2 == 0 else jnp.where(low, far, q)
        scores.append(jnp.dot(q, kt_ref[n, :, keys], preferred_element_type=F32))
    exps = [jnp.exp(s - jnp.max(s, axis=1, keepdims=True)).astype(BF16) for s in scores]
    outs = [jnp.dot(e, v_ref[n, keys, :], preferred_element_type=F32) for n, e in enumerate(exps)]
    done = []
    for p in range(pairs):
        even, odd = outs[2 * p], outs[2 * p + 1]
        top = jnp.where(low, even, odd)
        den = pltpu.roll(jnp.where(low, odd, even), 64, 1)
        done.append((top / den).astype(BF16))
    return jnp.concatenate(done, axis=1)


def attend_kernel(
    slots, seg_hbm, tok_hbm, wqkv_hbm, wout_hbm, wproj_hbm, ctx_ref, tok_ref, wout_ref, wproj_ref, kt_s, v_s,
    ql_ref, qml_ref, seg_ref, wqkv_ref, q_s, qm_s, sem,
):
    rows = tok_ref.shape[0]
    inner = ctx_ref.shape[1]
    head_dim = inner // HEADS
    pairs = HEADS // 2
    tile = min(256, rows)

    seg_copy = pltpu.make_async_copy(seg_hbm, seg_ref, sem.at[1 + rows // tile])
    seg_copy.start()
    w_copy = pltpu.make_async_copy(wqkv_hbm, wqkv_ref, sem.at[0])
    w_copy.start()

    def tok_copy(t):
        at = pl.ds(pl.multiple_of(t * tile, tile), tile)
        return pltpu.make_async_copy(tok_hbm.at[at, :], tok_ref.at[at, :], sem.at[t + 1])

    for t in range(rows // tile):
        tok_copy(t).start()
    seg_copy.wait()
    seg = seg_ref[...]

    sub = iota((128, rows), 0)
    slot = sub % head_dim
    far = jnp.where(slot < slots, jnp.where(slot == seg, 0.0, FAR), 0.0)
    qm_s[...] = far.T.astype(BF16)
    half = iota((head_dim, rows), 0)
    onehot = jnp.where(half == seg, 1.0, 0.0).astype(BF16)
    for p in range(pairs):
        kt_s[2 * p, head_dim:, :] = onehot
        kt_s[2 * p + 1, :head_dim, :] = onehot

    starts = [0] + [jnp.sum((seg < s).astype(F32)).astype(I32) for s in range(1, slots)] + [rows]

    w_copy.wait()

    def project(t, _):
        tok_copy(t).wait()
        at = pl.ds(pl.multiple_of(t * tile, tile), tile)
        low = iota((tile, 128), 1) < head_dim
        x = tok_ref[at, :]
        qkv = jnp.dot(x, wqkv_ref[...], preferred_element_type=F32)
        q_s[at, :] = (qkv[:, :inner].astype(BF16) * head_dim**-0.5).astype(BF16)
        for p in range(pairs):
            k = qkv[:, inner + p * 128 : inner + (p + 1) * 128]
            kt = k.T.astype(BF16)
            kt_s[2 * p, :head_dim, at] = kt[:head_dim]
            kt_s[2 * p + 1, head_dim:, at] = kt[head_dim:]
            v = qkv[:, 2 * inner + p * 128 : 2 * inner + (p + 1) * 128]
            v_s[2 * p, at, :] = jnp.where(low, v, 1.0).astype(BF16)
            v_s[2 * p + 1, at, :] = jnp.where(low, 1.0, v).astype(BF16)
        return 0

    lax.fori_loop(0, rows // tile, project, 0)

    later = [
        pltpu.make_async_copy(wout_hbm, wout_ref, sem.at[2 + rows // tile]),
        pltpu.make_async_copy(wproj_hbm, wproj_ref, sem.at[3 + rows // tile]),
    ]
    for copy in later:
        copy.start()

    def queries(t, _):
        q0 = t * TILE
        at = pl.ds(pl.multiple_of(q0, TILE), TILE)
        lo = jnp.int32(0)
        hi = jnp.int32(rows)
        for s in range(1, slots):
            lo = jnp.where(starts[s] <= q0, starts[s], lo)
        for s in range(slots - 1, 0, -1):
            hi = jnp.where(starts[s] >= q0 + TILE, starts[s], hi)
        lo = lo // 128 * 128
        needed = hi - lo
        spans = [w for w in (256, 384, 512, 640, 768, 896) if w < rows] + [rows]
        for below, w in zip([0] + spans, spans):

            @pl.when((needed > below) & (needed <= w))
            def _(w=w):
                first = 0 if w == rows else pl.multiple_of(jnp.minimum(lo, rows - w), 128)
                keys = pl.ds(first, w)
                ctx_ref[at, :] = context(q_s[at, :], qm_s[at, :], kt_s, v_s, keys)

        return 0

    lax.fori_loop(0, rows // TILE - 1, queries, 0)
    last = pl.ds(rows - TILE, TILE)
    ql_ref[...] = q_s[last, :]
    qml_ref[...] = qm_s[last, :]
    for copy in later:
        copy.wait()


def attend(seg, tokens, w_qkv, w_out, w_proj, slots):
    rows, width = tokens.shape
    inner = w_qkv.shape[1] // 3
    vmem = pl.BlockSpec(memory_space=pltpu.VMEM)
    hbm = pl.BlockSpec(memory_space=pltpu.HBM)
    return pl.pallas_call(
        functools.partial(attend_kernel, slots),
        name="attend",
        out_shape=[
            jax.ShapeDtypeStruct(x, BF16)
            for x in (
                (rows, inner), tokens.shape, w_out.shape, w_proj.shape,
                (HEADS, 128, rows), (HEADS, rows, 128), (TILE, inner), (TILE, 128),
            )
        ],
        in_specs=[hbm] * 5,
        out_specs=[vmem] * 8,
        scratch_shapes=[
            pltpu.VMEM((1, rows), I32),
            pltpu.VMEM((width, 3 * inner), BF16),
            pltpu.VMEM((rows, inner), BF16),
            pltpu.VMEM((rows, 128), BF16),
            pltpu.SemaphoreType.DMA((4 + rows // min(256, rows),)),
        ],
        compiler_params=pltpu.CompilerParams(vmem_limit_bytes=40 * 2**20),
        cost_estimate=pl.CostEstimate(flops=8 * 10**9, bytes_accessed=6 * 2**20, transcendentals=4 * 10**6),
    )(seg, tokens, w_qkv, w_out, w_proj)


def halves(x):
    hi = x.astype(BF16)
    return hi, (x - hi.astype(F32)).astype(BF16)


def loss_kernel(
    n_z, n_y, n_x, slots,
    counts_ref, pos_ref, seg_ref, tok_ref, ctx_ref, wout_ref, gain_ref, w_ref,
    kt_ref, v_ref, ql_ref, qml_ref, loss_ref, grad_ref,
    mine_s, colp, rowp, drow, dcol, yrecv, ysend, mdr, mdc,
    p_s, unit_s, emb_s, wt_s,
    s_colp, r_colp, s_rowp, r_rowp, s_dr, r_dr, s_dc, r_dc, s_y, r_y,
):
    n_a, n_b = n_z * 2, n_y * n_x
    me = lax.axis_index("dp")
    core, b, z = me % 2, (me // 2) % n_b, me // (2 * n_b)
    a = z * 2 + core
    rows, width = tok_ref.shape
    embed = w_ref.shape[1]
    r_rows = slots * n_b
    c_cols = slots * n_a

    def ring(d, n):
        return min(d, n - d)

    row_peers = []
    for dy in range(n_y):
        for dx in range(n_x):
            o = (b // n_x + dy) % n_y * n_x + (b % n_x + dx) % n_x
            row_peers.append((2 * ring(dy, n_y) + 2 * ring(dx, n_x), o, z * (2 * n_b) + o * 2 + core))
    col_peers = []
    for dz in range(n_z):
        for dc in range(2):
            o = (z + dz) % n_z * 2 + (core + dc) % 2
            col_peers.append((2 * ring(dz, n_z) + dc, o, (o // 2) * (2 * n_b) + b * 2 + o % 2))
    row_peers, col_peers = row_peers[1:], col_peers[1:]

    barrier = pltpu.get_barrier_semaphore()
    for _, _, device in row_peers + col_peers:
        pl.semaphore_signal(barrier, inc=1, device_id=(device,), device_id_type=MESH)

    def exchange(peers, mine, source, dest, send, recv):
        out = []
        for k, (hops, o, device) in enumerate(peers):
            out.append((
                hops,
                functools.partial(
                    pltpu.make_async_remote_copy, src_ref=source(o), dst_ref=dest.at[mine], send_sem=send.at[k],
                    recv_sem=recv.at[mine], device_id=(device,), device_id_type=MESH,
                ),
                functools.partial(
                    pltpu.make_async_remote_copy, src_ref=source(o), dst_ref=dest.at[o], send_sem=send.at[k],
                    recv_sem=recv.at[o], device_id=(device,), device_id_type=MESH,
                ),
            ))
        return sorted(out, key=lambda c: -c[0])

    def start(*exchanges):
        for _, copy, _ in sorted(sum(exchanges, []), key=lambda c: -c[0]):
            copy().start()

    def arrive(exchange):
        for _, _, copy in reversed(exchange):
            copy().wait_recv()

    x_col = exchange(col_peers, a, lambda o: mine_s, colp, s_colp, r_colp)
    x_row = exchange(row_peers, b, lambda o: mine_s, rowp, s_rowp, r_rowp)
    x_dr = exchange(row_peers, b, lambda o: mdr, drow, s_dr, r_dr)
    x_dc = exchange(col_peers, a, lambda o: mdc, dcol, s_dc, r_dc)
    x_y = exchange(row_peers, b, lambda o: ysend.at[o], yrecv, s_y, r_y)

    s_id = iota((slots, 1), 0)
    lane = iota((slots, 128), 1)
    n_devices = counts_ref.shape[1]
    my_count = jnp.sum(jnp.where(iota((1, n_devices), 1) == me, counts_ref[...], 0).astype(F32), axis=1, keepdims=True)
    live_own = (s_id.astype(F32) < my_count).astype(F32)
    diagonal = iota((slots, slots), 0) == iota((slots, slots), 1)

    def down(values):
        return jnp.sum(jnp.where(diagonal, values.astype(F32), 0.0), axis=1, keepdims=True)

    places = pos_ref[...]
    side = jnp.where(lane == 0, down(places >> 5), jnp.where(lane == 1, down(places & 31), 0.0))
    side = jnp.where(lane == 2, live_own, side)
    mine_s[:, width:] = side.astype(BF16)

    last = context(ql_ref[...], qml_ref[...], kt_ref, v_ref, pl.ds(0, rows))

    tile = min(256, rows)

    def mix_in(t):
        at = pl.ds(t * tile, tile)
        if t == rows // tile - 1:
            rest = jnp.concatenate([ctx_ref[pl.ds(t * tile, tile - TILE), :], last], axis=0)
        else:
            rest = ctx_ref[at, :]
        return tok_ref[at, :].astype(F32) + jnp.dot(rest, wout_ref[...], preferred_element_type=F32)

    def norm(resid):
        centre = resid - jnp.sum(resid, axis=1, keepdims=True) * (1.0 / width)
        variance = jnp.sum(centre * centre, axis=1, keepdims=True) * (1.0 / width)
        return (centre * lax.rsqrt(variance + 1e-05) * gain_ref[...]).astype(BF16)

    def pool(t, hidden):
        member = (iota((16, tile), 0) == seg_ref[:, pl.ds(t * tile, tile)]).astype(F32).astype(BF16)
        return jnp.dot(member, hidden, preferred_element_type=F32)

    resids = [mix_in(t) for t in range(rows // tile)]
    sums = sum(pool(t, norm(resid)) for t, resid in enumerate(resids))
    sizes = jnp.sum((iota((16, rows), 0) == seg_ref[...]).astype(F32), axis=1, keepdims=True)
    pooled = (sums[:slots] / sizes[:slots]).astype(BF16)
    mine_s[:, :width] = pooled

    pl.semaphore_wait(barrier, n_a + n_b - 2)
    start(x_col, x_row)

    proj = jnp.dot(pooled, w_ref[...], preferred_element_type=F32)
    rnorm = lax.rsqrt(jnp.sum(proj * proj, axis=1, keepdims=True) + 1e-06)
    unit_s[...] = proj * rnorm

    def turn(j, _):
        at = pl.ds(pl.multiple_of(j * 128, 128), 128)
        wt_s[at, :] = w_ref[:, at].T
        return 0

    lax.fori_loop(0, embed // 128, turn, 0)
    colp[a] = mine_s[...]
    rowp[b] = mine_s[...]
    p_s[...] = jnp.zeros_like(p_s)
    arrive(x_row)
    for o in range(n_b):
        p_s[128 + o * slots : 128 + (o + 1) * slots, :] = rowp[o].astype(F32)
    arrive(x_col)
    for o in range(n_a):
        p_s[o * slots : (o + 1) * slots, :] = colp[o].astype(F32)

    proj_all = jnp.dot(p_s[:, :width].astype(BF16), w_ref[...], preferred_element_type=F32)
    rnorm_all = lax.rsqrt(jnp.sum(proj_all * proj_all, axis=1, keepdims=True) + 1e-06)
    emb_s[...] = (proj_all * rnorm_all).astype(BF16)
    emb_j = emb_s[:128, :]
    logits = SCALE * lax.dot_general(emb_s[128 : 128 + r_rows, :], emb_j, NT, preferred_element_type=F32)

    r = iota((r_rows, 128), 0)
    c = iota((r_rows, 128), 1)
    id_i = (z * (2 * n_b) + (r // slots) * 2 + core) * slots + r % slots
    o_j = c // slots
    id_j = ((o_j // 2) * (2 * n_b) + b * 2 + o_j % 2) * slots + c % slots
    eye = r == c
    square = iota((128, 128), 0) == iota((128, 128), 1)

    def along(column):
        return jnp.sum(jnp.where(square, column, 0.0), axis=0, keepdims=True)

    side_j = p_s[:128, width:]
    side_i = p_s[128 : 128 + r_rows, width:]
    pos_i, live_i = side_i[:, 0:1] * 32.0 + side_i[:, 1:2], side_i[:, 2:3] > 0.5
    pos_j, live_j = along(side_j[:, 0:1] * 32.0 + side_j[:, 1:2]), along(side_j[:, 2:3]) > 0.5
    inside = (c < c_cols) & (id_i != id_j)
    expd = jnp.exp(logits)
    exp_i = jnp.where(inside & live_j, expd, 0.0)
    exp_j = jnp.where(inside & live_i, expd, 0.0)
    hit_i = (pos_i == id_j.astype(F32)) & (c < c_cols)
    hit_j = (pos_j == id_i.astype(F32)) & (c < c_cols)
    part_i = jnp.sum(exp_i, axis=1, keepdims=True)
    picked = jnp.sum(jnp.where(hit_i, logits, 0.0), axis=1, keepdims=True)
    mdc[...] = jnp.sum(exp_j, axis=0, keepdims=True)
    mdr[0:1, :] = jnp.sum(jnp.where(eye, part_i, 0.0), axis=0, keepdims=True)
    mdr[1:2, :] = jnp.sum(jnp.where(eye, picked, 0.0), axis=0, keepdims=True)
    start(x_dr, x_dc)
    drow[b] = mdr[...]
    dcol[a] = mdc[...]
    arrive(x_dr)
    arrive(x_dc)
    sums_i = jnp.sum(drow[...], axis=0)
    den_j = jnp.sum(dcol[...], axis=0)
    den_i = jnp.sum(jnp.where(eye, sums_i[0:1], 0.0), axis=1, keepdims=True)
    w_i = jnp.where(live_i, exp_i / den_i - hit_i.astype(F32), 0.0)
    den_j = jnp.where(den_j > 0.0, den_j, 1.0)
    w_j = jnp.where(live_j & (c < c_cols), exp_j / den_j - hit_j.astype(F32), 0.0)
    mix = jnp.concatenate(halves(w_i + w_j), axis=0)
    y = jnp.dot(mix, emb_j, preferred_element_type=F32)
    y = (y[:r_rows] + y[r_rows:]).astype(BF16)
    for o in range(n_b):
        ysend[o] = y[o * slots : (o + 1) * slots]
    start(x_y)
    yrecv[b] = ysend[b]

    table = jnp.log(sums_i[0:1]) - sums_i[1:2]
    mine = jnp.sum(jnp.where(lane == b * slots + iota((slots, 128), 0), table, 0.0), axis=1, keepdims=True)
    mine = jnp.where(live_own > 0.5, mine, 0.0)
    loss_lane = jnp.sum(jnp.where(lane == iota((slots, 128), 0), mine, 0.0), axis=0, keepdims=True)
    loss_ref[...] = loss_lane[:, :slots]

    arrive(x_y)
    d_emb = SCALE * jnp.sum(yrecv[...].astype(F32), axis=0)
    own = unit_s[...]
    radial = jnp.sum(d_emb * own, axis=1, keepdims=True)
    d_proj = ((d_emb - radial * own) * rnorm).astype(BF16)
    grad_ref[...] = jnp.dot(d_proj, wt_s[...], preferred_element_type=F32)
    for x in (x_col, x_row, x_dr, x_dc, x_y):
        for _, copy, _ in x:
            copy().wait_send()


def contrast(counts, positives, seg, tokens, ctx, w_out, gain, w_proj, last, n_z, n_y, n_x):
    slots = positives.shape[1]
    n_a, n_b = n_z * 2, n_y * n_x
    width, embed = w_proj.shape
    vmem = pl.BlockSpec(memory_space=pltpu.VMEM)
    sems = [pltpu.SemaphoreType.DMA((n,)) for n in (n_a, n_b, n_b, n_a, n_b) for _ in range(2)]
    return pl.pallas_call(
        functools.partial(loss_kernel, n_z, n_y, n_x, slots),
        name="contrast",
        out_shape=(jax.ShapeDtypeStruct((1, slots), F32), jax.ShapeDtypeStruct((slots, width), F32)),
        in_specs=[vmem] * 12,
        out_specs=(vmem, vmem),
        scratch_shapes=[
            pltpu.VMEM((slots, width + 128), BF16),
            pltpu.VMEM((n_a, slots, width + 128), BF16),
            pltpu.VMEM((n_b, slots, width + 128), BF16),
            pltpu.VMEM((n_b, 2, 128), F32),
            pltpu.VMEM((n_a, 1, 128), F32),
            pltpu.VMEM((n_b, slots, embed), BF16),
            pltpu.VMEM((n_b, slots, embed), BF16),
            pltpu.VMEM((2, 128), F32),
            pltpu.VMEM((1, 128), F32),
            pltpu.VMEM((128 + slots * n_b, width + 128), F32),
            pltpu.VMEM((slots, embed), F32),
            pltpu.VMEM((128 + slots * n_b, embed), BF16),
            pltpu.VMEM((embed, width), BF16),
            *sems,
        ],
        compiler_params=pltpu.CompilerParams(collective_id=0, has_side_effects=True, vmem_limit_bytes=40 * 2**20),
    )(counts, positives, seg, tokens, ctx, w_out, gain, w_proj, *last)


def deliver_kernel(loss_ref, grad_ref, loss_hbm, grad_hbm, sem):
    copies = [pltpu.make_async_copy(loss_ref, loss_hbm, sem.at[0]), pltpu.make_async_copy(grad_ref, grad_hbm, sem.at[1])]
    for copy in copies:
        copy.start()
    for copy in copies:
        copy.wait()


def deliver(loss, grad):
    vmem = pl.BlockSpec(memory_space=pltpu.VMEM)
    hbm = pl.BlockSpec(memory_space=pltpu.HBM)
    return pl.pallas_call(
        deliver_kernel,
        name="deliver",
        out_shape=(jax.ShapeDtypeStruct(loss.shape, F32), jax.ShapeDtypeStruct(grad.shape, F32)),
        in_specs=[vmem, vmem],
        out_specs=(hbm, hbm),
        scratch_shapes=[pltpu.SemaphoreType.DMA((2,))],
        compiler_params=pltpu.CompilerParams(vmem_limit_bytes=2**20),
    )(loss, grad)


def body(grid, tokens, seg_ids, counts, positives, w_qkv, w_out, ln_gain, w_proj):
    slots = positives.shape[0]
    in_hbm = functools.partial(pltpu.with_memory_space_constraint, memory_space=pltpu.HBM)
    ctx, tokens, w_out, w_proj, *last = attend(*map(in_hbm, (seg_ids, tokens, w_qkv, w_out, w_proj)), slots)
    loss, grad = contrast(counts[None, :], positives[None, :], seg_ids, tokens, ctx, w_out, ln_gain[None, :], w_proj, last, *grid)
    loss, grad = deliver(loss, grad)
    return loss.reshape(slots), grad


def solution(mesh):
    grid = (mesh.size // 32, 4, 4)
    return jax.shard_map(
        functools.partial(body, grid),
        mesh=mesh,
        in_specs=(P("dp", None), P("dp", None), P(), P("dp"), P(), P(), P(), P()),
        out_specs=(P("dp"), P("dp", None)),
        check_vma=False,
    )
```

```python
import functools

import jax
import jax.numpy as jnp
from jax import lax
from jax.experimental import pallas as pl
from jax.experimental.pallas import tpu as pltpu
from jax.sharding import PartitionSpec as P

HEADS = 8
SCALE = 20.0
FAR = -1e30
MESH = pl.DeviceIdType.MESH
F32 = jnp.float32
BF16 = jnp.bfloat16
I32 = jnp.int32
NT = (((1,), (1,)), ((), ()))


def iota(shape, dim):
    return lax.broadcasted_iota(I32, shape, dim)


def attend_kernel(
    slots, seg_hbm, tok_hbm, wqkv_hbm, wout_hbm, wproj_hbm, ctx_ref, tok_ref, wout_ref, wproj_ref, seg_ref, wqkv_ref, q_s, kt_s, v_s, qm_s, sem,
):
    rows = tok_ref.shape[0]
    inner = ctx_ref.shape[1]
    head_dim = inner // HEADS
    pairs = HEADS // 2
    tile = min(256, rows)
    qtile = 128

    seg_copy = pltpu.make_async_copy(seg_hbm, seg_ref, sem.at[1 + rows // tile])
    seg_copy.start()
    w_copy = pltpu.make_async_copy(wqkv_hbm, wqkv_ref, sem.at[0])
    w_copy.start()

    def tok_copy(t):
        at = pl.ds(pl.multiple_of(t * tile, tile), tile)
        return pltpu.make_async_copy(tok_hbm.at[at, :], tok_ref.at[at, :], sem.at[t + 1])

    for t in range(rows // tile):
        tok_copy(t).start()
    seg_copy.wait()
    seg = seg_ref[...]

    sub = iota((128, rows), 0)
    slot = sub % head_dim
    far = jnp.where(slot < slots, jnp.where(slot == seg, 0.0, FAR), 0.0)
    qm_s[...] = far.T.astype(BF16)
    half = iota((head_dim, rows), 0)
    onehot = jnp.where(half == seg, 1.0, 0.0).astype(BF16)
    for p in range(pairs):
        kt_s[2 * p, head_dim:, :] = onehot
        kt_s[2 * p + 1, :head_dim, :] = onehot

    starts = [0] + [jnp.sum((seg < s).astype(F32)).astype(I32) for s in range(1, slots)] + [rows]

    w_copy.wait()

    def project(t, _):
        tok_copy(t).wait()
        at = pl.ds(pl.multiple_of(t * tile, tile), tile)
        low = iota((tile, 128), 1) < head_dim
        x = tok_ref[at, :]
        qkv = jnp.dot(x, wqkv_ref[...], preferred_element_type=F32)
        q_s[at, :] = (qkv[:, :inner].astype(BF16) * head_dim**-0.5).astype(BF16)
        for p in range(pairs):
            k = qkv[:, inner + p * 128 : inner + (p + 1) * 128]
            kt = k.T.astype(BF16)
            kt_s[2 * p, :head_dim, at] = kt[:head_dim]
            kt_s[2 * p + 1, head_dim:, at] = kt[head_dim:]
            v = qkv[:, 2 * inner + p * 128 : 2 * inner + (p + 1) * 128]
            v_s[2 * p, at, :] = jnp.where(low, v, 1.0).astype(BF16)
            v_s[2 * p + 1, at, :] = jnp.where(low, 1.0, v).astype(BF16)
        return 0

    lax.fori_loop(0, rows // tile, project, 0)

    later = [
        pltpu.make_async_copy(wout_hbm, wout_ref, sem.at[2 + rows // tile]),
        pltpu.make_async_copy(wproj_hbm, wproj_ref, sem.at[3 + rows // tile]),
    ]
    for copy in later:
        copy.start()

    def window(tiles, span):
        low = iota((qtile, 128), 1) < head_dim
        scores = []
        for at, first in tiles:
            qm = qm_s[at, :]
            for n in range(HEADS):
                q = q_s[at, n // 2 * 128 : (n // 2 + 1) * 128]
                q = jnp.where(low, q, qm) if n % 2 == 0 else jnp.where(low, qm, q)
                scores.append(jnp.dot(q, kt_s[n, :, pl.ds(first, span)], preferred_element_type=F32))
        exps = [jnp.exp(s - jnp.max(s, axis=1, keepdims=True)).astype(BF16) for s in scores]
        outs = []
        for i, (at, first) in enumerate(tiles):
            for n in range(HEADS):
                outs.append(jnp.dot(exps[i * HEADS + n], v_s[n, pl.ds(first, span), :], preferred_element_type=F32))
        for i, (at, first) in enumerate(tiles):
            for p in range(pairs):
                even, odd = outs[i * HEADS + 2 * p], outs[i * HEADS + 2 * p + 1]
                top = jnp.where(low, even, odd)
                den = pltpu.roll(jnp.where(low, odd, even), head_dim, 1)
                ctx_ref[at, p * 128 : (p + 1) * 128] = (top / den).astype(BF16)

    group = 1

    def queries(t, _):
        los, width_needed = [], jnp.int32(0)
        for i in range(group):
            q0 = (t * group + i) * qtile
            lo = jnp.int32(0)
            hi = jnp.int32(rows)
            for s in range(1, slots):
                lo = jnp.where(starts[s] <= q0, starts[s], lo)
            for s in range(slots - 1, 0, -1):
                hi = jnp.where(starts[s] >= q0 + qtile, starts[s], hi)
            lo = lo // 128 * 128
            los.append(lo)
            width_needed = jnp.maximum(width_needed, hi - lo)
        spans = [w for w in (256, 384, 512, 640, 768, 896) if w < rows] + [rows]
        for below, w in zip([0] + spans, spans):

            @pl.when((width_needed > below) & (width_needed <= w))
            def _(w=w):
                tiles = []
                for i in range(group):
                    at = pl.ds(pl.multiple_of((t * group + i) * qtile, qtile), qtile)
                    tiles.append((at, 0 if w == rows else pl.multiple_of(jnp.minimum(los[i], rows - w), 128)))
                window(tiles, w)

        return 0

    lax.fori_loop(0, rows // (qtile * group), queries, 0)
    for copy in later:
        copy.wait()


def attend(seg, tokens, w_qkv, w_out, w_proj, slots):
    rows, width = tokens.shape
    inner = w_qkv.shape[1] // 3
    vmem = pl.BlockSpec(memory_space=pltpu.VMEM)
    hbm = pl.BlockSpec(memory_space=pltpu.HBM)
    return pl.pallas_call(
        functools.partial(attend_kernel, slots),
        name="attend",
        out_shape=[jax.ShapeDtypeStruct(x, BF16) for x in ((rows, inner), tokens.shape, w_out.shape, w_proj.shape)],
        in_specs=[hbm] * 5,
        out_specs=[vmem] * 4,
        scratch_shapes=[
            pltpu.VMEM((1, rows), I32),
            pltpu.VMEM((width, 3 * inner), BF16),
            pltpu.VMEM((rows, inner), BF16),
            pltpu.VMEM((HEADS, 128, rows), BF16),
            pltpu.VMEM((HEADS, rows, 128), BF16),
            pltpu.VMEM((rows, 128), BF16),
            pltpu.SemaphoreType.DMA((4 + rows // min(256, rows),)),
        ],
        compiler_params=pltpu.CompilerParams(vmem_limit_bytes=40 * 2**20),
        cost_estimate=pl.CostEstimate(flops=8 * 10**9, bytes_accessed=6 * 2**20, transcendentals=4 * 10**6),
    )(seg, tokens, w_qkv, w_out, w_proj)


def halves(x):
    hi = x.astype(BF16)
    return hi, (x - hi.astype(F32)).astype(BF16)


def loss_kernel(
    n_z, n_y, n_x, slots,
    counts_ref, pos_ref, seg_ref, tok_ref, ctx_ref, wout_ref, gain_ref, w_ref, loss_ref, grad_ref,
    mine_s, colp, rowp, drow, dcol, yrecv, ysend, mdr, mdc,
    p_s, unit_s, emb_s, wt_s,
    s_colp, r_colp, s_rowp, r_rowp, s_dr, r_dr, s_dc, r_dc, s_y, r_y,
):
    n_a, n_b = n_z * 2, n_y * n_x
    me = lax.axis_index("dp")
    core, b, z = me % 2, (me // 2) % n_b, me // (2 * n_b)
    a = z * 2 + core
    rows, width = tok_ref.shape
    embed = w_ref.shape[1]
    r_rows = slots * n_b
    c_cols = slots * n_a

    def ring(d, n):
        return min(d, n - d)

    row_peers = []
    for dy in range(n_y):
        for dx in range(n_x):
            o = (b // n_x + dy) % n_y * n_x + (b % n_x + dx) % n_x
            row_peers.append((2 * ring(dy, n_y) + 2 * ring(dx, n_x), o, z * (2 * n_b) + o * 2 + core))
    col_peers = []
    for dz in range(n_z):
        for dc in range(2):
            o = (z + dz) % n_z * 2 + (core + dc) % 2
            col_peers.append((2 * ring(dz, n_z) + dc, o, (o // 2) * (2 * n_b) + b * 2 + o % 2))
    row_peers, col_peers = row_peers[1:], col_peers[1:]

    barrier = pltpu.get_barrier_semaphore()
    for _, _, device in row_peers + col_peers:
        pl.semaphore_signal(barrier, inc=1, device_id=(device,), device_id_type=MESH)

    def exchange(peers, mine, source, dest, send, recv):
        out = []
        for k, (hops, o, device) in enumerate(peers):
            out.append((
                hops,
                functools.partial(
                    pltpu.make_async_remote_copy, src_ref=source(o), dst_ref=dest.at[mine], send_sem=send.at[k],
                    recv_sem=recv.at[mine], device_id=(device,), device_id_type=MESH,
                ),
                functools.partial(
                    pltpu.make_async_remote_copy, src_ref=source(o), dst_ref=dest.at[o], send_sem=send.at[k],
                    recv_sem=recv.at[o], device_id=(device,), device_id_type=MESH,
                ),
            ))
        return sorted(out, key=lambda c: -c[0])

    def start(*exchanges):
        for _, copy, _ in sorted(sum(exchanges, []), key=lambda c: -c[0]):
            copy().start()

    def arrive(exchange):
        for _, _, copy in reversed(exchange):
            copy().wait_recv()

    x_col = exchange(col_peers, a, lambda o: mine_s, colp, s_colp, r_colp)
    x_row = exchange(row_peers, b, lambda o: mine_s, rowp, s_rowp, r_rowp)
    x_dr = exchange(row_peers, b, lambda o: mdr, drow, s_dr, r_dr)
    x_dc = exchange(col_peers, a, lambda o: mdc, dcol, s_dc, r_dc)
    x_y = exchange(row_peers, b, lambda o: ysend.at[o], yrecv, s_y, r_y)

    s_id = iota((slots, 1), 0)
    lane = iota((slots, 128), 1)
    n_devices = counts_ref.shape[1]
    my_count = jnp.sum(jnp.where(iota((1, n_devices), 1) == me, counts_ref[...], 0).astype(F32), axis=1, keepdims=True)
    live_own = (s_id.astype(F32) < my_count).astype(F32)
    diagonal = iota((slots, slots), 0) == iota((slots, slots), 1)

    def down(values):
        return jnp.sum(jnp.where(diagonal, values.astype(F32), 0.0), axis=1, keepdims=True)

    places = pos_ref[...]
    side = jnp.where(lane == 0, down(places >> 5), jnp.where(lane == 1, down(places & 31), 0.0))
    side = jnp.where(lane == 2, live_own, side)
    mine_s[:, width:] = side.astype(BF16)

    tile = min(256, rows)

    def mix_in(t):
        at = pl.ds(t * tile, tile)
        return tok_ref[at, :].astype(F32) + jnp.dot(ctx_ref[at, :], wout_ref[...], preferred_element_type=F32)

    def norm(resid):
        centre = resid - jnp.sum(resid, axis=1, keepdims=True) * (1.0 / width)
        variance = jnp.sum(centre * centre, axis=1, keepdims=True) * (1.0 / width)
        return (centre * lax.rsqrt(variance + 1e-05)).astype(BF16)

    def pool(t, hidden):
        member = (iota((16, tile), 0) == seg_ref[:, pl.ds(t * tile, tile)]).astype(F32).astype(BF16)
        return jnp.dot(member, hidden, preferred_element_type=F32)

    resids = [mix_in(t) for t in range(rows // tile)]
    sums = sum(pool(t, norm(resid)) for t, resid in enumerate(resids))
    sizes = jnp.sum((iota((16, rows), 0) == seg_ref[...]).astype(F32), axis=1, keepdims=True)
    pooled = (sums[:slots] / sizes[:slots] * gain_ref[...]).astype(BF16)
    mine_s[:, :width] = pooled

    pl.semaphore_wait(barrier, n_a + n_b - 2)
    start(x_col, x_row)

    proj = jnp.dot(pooled, w_ref[...], preferred_element_type=F32)
    rnorm = lax.rsqrt(jnp.sum(proj * proj, axis=1, keepdims=True) + 1e-06)
    unit_s[...] = proj * rnorm

    def turn(j, _):
        at = pl.ds(pl.multiple_of(j * 128, 128), 128)
        wt_s[at, :] = w_ref[:, at].T
        return 0

    lax.fori_loop(0, embed // 128, turn, 0)
    colp[a] = mine_s[...]
    rowp[b] = mine_s[...]
    p_s[...] = jnp.zeros_like(p_s)
    emb_s[...] = jnp.zeros_like(emb_s)

    def embed_rows(first, count):
        at = pl.ds(first, count)
        proj_at = jnp.dot(p_s[at, :width].astype(BF16), w_ref[...], preferred_element_type=F32)
        rnorm_at = lax.rsqrt(jnp.sum(proj_at * proj_at, axis=1, keepdims=True) + 1e-06)
        emb_s[at, :] = (proj_at * rnorm_at).astype(BF16)

    arrive(x_row)
    for o in range(n_b):
        p_s[128 + o * slots : 128 + (o + 1) * slots, :] = rowp[o].astype(F32)
    embed_rows(128, r_rows)
    arrive(x_col)
    for o in range(n_a):
        p_s[o * slots : (o + 1) * slots, :] = colp[o].astype(F32)

    embed_rows(0, c_cols)
    emb_j = emb_s[:128, :]
    logits = SCALE * lax.dot_general(emb_s[128 : 128 + r_rows, :], emb_j, NT, preferred_element_type=F32)

    r = iota((r_rows, 128), 0)
    c = iota((r_rows, 128), 1)
    id_i = (z * (2 * n_b) + (r // slots) * 2 + core) * slots + r % slots
    o_j = c // slots
    id_j = ((o_j // 2) * (2 * n_b) + b * 2 + o_j % 2) * slots + c % slots
    eye = r == c
    square = iota((128, 128), 0) == iota((128, 128), 1)

    def along(column):
        return jnp.sum(jnp.where(square, column, 0.0), axis=0, keepdims=True)

    side_j = p_s[:128, width:]
    side_i = p_s[128 : 128 + r_rows, width:]
    pos_i, live_i = side_i[:, 0:1] * 32.0 + side_i[:, 1:2], side_i[:, 2:3] > 0.5
    pos_j, live_j = along(side_j[:, 0:1] * 32.0 + side_j[:, 1:2]), along(side_j[:, 2:3]) > 0.5
    inside = (c < c_cols) & (id_i != id_j)
    expd = jnp.exp(logits)
    exp_i = jnp.where(inside & live_j, expd, 0.0)
    exp_j = jnp.where(inside & live_i, expd, 0.0)
    hit_i = (pos_i == id_j.astype(F32)) & (c < c_cols)
    hit_j = (pos_j == id_i.astype(F32)) & (c < c_cols)
    part_i = jnp.sum(exp_i, axis=1, keepdims=True)
    picked = jnp.sum(jnp.where(hit_i, logits, 0.0), axis=1, keepdims=True)
    mdc[...] = jnp.sum(exp_j, axis=0, keepdims=True)
    mdr[0:1, :] = jnp.sum(jnp.where(eye, part_i, 0.0), axis=0, keepdims=True)
    mdr[1:2, :] = jnp.sum(jnp.where(eye, picked, 0.0), axis=0, keepdims=True)
    start(x_dr, x_dc)
    drow[b] = mdr[...]
    dcol[a] = mdc[...]
    arrive(x_dr)
    arrive(x_dc)
    sums_i = jnp.sum(drow[...], axis=0)
    den_j = jnp.sum(dcol[...], axis=0)
    den_i = jnp.sum(jnp.where(eye, sums_i[0:1], 0.0), axis=1, keepdims=True)
    w_i = jnp.where(live_i, exp_i / den_i - hit_i.astype(F32), 0.0)
    den_j = jnp.where(den_j > 0.0, den_j, 1.0)
    w_j = jnp.where(live_j & (c < c_cols), exp_j / den_j - hit_j.astype(F32), 0.0)
    mix = jnp.concatenate(halves(w_i + w_j), axis=0)
    y = jnp.dot(mix, emb_j, preferred_element_type=F32)
    y = (y[:r_rows] + y[r_rows:]).astype(BF16)
    for o in range(n_b):
        ysend[o] = y[o * slots : (o + 1) * slots]
    start(x_y)
    yrecv[b] = ysend[b]

    table = jnp.log(sums_i[0:1]) - sums_i[1:2]
    mine = jnp.sum(jnp.where(lane == b * slots + iota((slots, 128), 0), table, 0.0), axis=1, keepdims=True)
    mine = jnp.where(live_own > 0.5, mine, 0.0)
    loss_lane = jnp.sum(jnp.where(lane == iota((slots, 128), 0), mine, 0.0), axis=0, keepdims=True)
    loss_ref[...] = loss_lane[:, :slots]

    arrive(x_y)
    d_emb = SCALE * jnp.sum(yrecv[...].astype(F32), axis=0)
    own = unit_s[...]
    radial = jnp.sum(d_emb * own, axis=1, keepdims=True)
    d_proj = ((d_emb - radial * own) * rnorm).astype(BF16)
    grad_ref[...] = jnp.dot(d_proj, wt_s[...], preferred_element_type=F32)
    for x in (x_col, x_row, x_dr, x_dc, x_y):
        for _, copy, _ in x:
            copy().wait_send()


def contrast(counts, positives, seg, tokens, ctx, w_out, gain, w_proj, n_z, n_y, n_x):
    slots = positives.shape[1]
    n_a, n_b = n_z * 2, n_y * n_x
    width, embed = w_proj.shape
    vmem = pl.BlockSpec(memory_space=pltpu.VMEM)
    sems = [pltpu.SemaphoreType.DMA((n,)) for n in (n_a, n_b, n_b, n_a, n_b) for _ in range(2)]
    return pl.pallas_call(
        functools.partial(loss_kernel, n_z, n_y, n_x, slots),
        name="contrast",
        out_shape=(jax.ShapeDtypeStruct((1, slots), F32), jax.ShapeDtypeStruct((slots, width), F32)),
        in_specs=[vmem] * 8,
        out_specs=(vmem, vmem),
        scratch_shapes=[
            pltpu.VMEM((slots, width + 128), BF16),
            pltpu.VMEM((n_a, slots, width + 128), BF16),
            pltpu.VMEM((n_b, slots, width + 128), BF16),
            pltpu.VMEM((n_b, 2, 128), F32),
            pltpu.VMEM((n_a, 1, 128), F32),
            pltpu.VMEM((n_b, slots, embed), BF16),
            pltpu.VMEM((n_b, slots, embed), BF16),
            pltpu.VMEM((2, 128), F32),
            pltpu.VMEM((1, 128), F32),
            pltpu.VMEM((128 + slots * n_b, width + 128), F32),
            pltpu.VMEM((slots, embed), F32),
            pltpu.VMEM((128 + slots * n_b, embed), BF16),
            pltpu.VMEM((embed, width), BF16),
            *sems,
        ],
        compiler_params=pltpu.CompilerParams(collective_id=0, has_side_effects=True, vmem_limit_bytes=40 * 2**20),
    )(counts, positives, seg, tokens, ctx, w_out, gain, w_proj)


def deliver_kernel(loss_ref, grad_ref, loss_hbm, grad_hbm, sem):
    copies = [pltpu.make_async_copy(loss_ref, loss_hbm, sem.at[0]), pltpu.make_async_copy(grad_ref, grad_hbm, sem.at[1])]
    for copy in copies:
        copy.start()
    for copy in copies:
        copy.wait()


def deliver(loss, grad):
    vmem = pl.BlockSpec(memory_space=pltpu.VMEM)
    hbm = pl.BlockSpec(memory_space=pltpu.HBM)
    return pl.pallas_call(
        deliver_kernel,
        name="deliver",
        out_shape=(jax.ShapeDtypeStruct(loss.shape, F32), jax.ShapeDtypeStruct(grad.shape, F32)),
        in_specs=[vmem, vmem],
        out_specs=(hbm, hbm),
        scratch_shapes=[pltpu.SemaphoreType.DMA((2,))],
        compiler_params=pltpu.CompilerParams(vmem_limit_bytes=2**20),
    )(loss, grad)


def body(grid, tokens, seg_ids, counts, positives, w_qkv, w_out, ln_gain, w_proj):
    slots = positives.shape[0]
    in_hbm = functools.partial(pltpu.with_memory_space_constraint, memory_space=pltpu.HBM)
    ctx, tokens, w_out, w_proj = attend(*map(in_hbm, (seg_ids, tokens, w_qkv, w_out, w_proj)), slots)
    loss, grad = contrast(counts[None, :], positives[None, :], seg_ids, tokens, ctx, w_out, ln_gain[None, :], w_proj, *grid)
    loss, grad = deliver(loss, grad)
    return loss.reshape(slots), grad


def solution(mesh):
    grid = (mesh.size // 32, 4, 4)
    return jax.shard_map(
        functools.partial(body, grid),
        mesh=mesh,
        in_specs=(P("dp", None), P("dp", None), P(), P("dp"), P(), P(), P(), P()),
        out_specs=(P("dp"), P("dp", None)),
        check_vma=False,
    )
```

```python
import functools

import jax
import jax.numpy as jnp
from jax import lax
from jax.experimental import pallas as pl
from jax.experimental.pallas import tpu as pltpu
from jax.sharding import PartitionSpec as P

HEADS = 8
SCALE = 20.0
FAR = -1e30
MESH = pl.DeviceIdType.MESH
F32 = jnp.float32
BF16 = jnp.bfloat16
I32 = jnp.int32
NT = (((1,), (1,)), ((), ()))


def iota(shape, dim):
    return lax.broadcasted_iota(I32, shape, dim)


def attend_kernel(
    slots, seg_hbm, tok_hbm, wqkv_hbm, wout_hbm, wproj_hbm, ctx_ref, tok_ref, wout_ref, wproj_ref, seg_ref, wqkv_ref, q_s, kt_s, v_s, qm_s, sem,
):
    rows = tok_ref.shape[0]
    inner = ctx_ref.shape[1]
    head_dim = inner // HEADS
    pairs = HEADS // 2
    tile = min(256, rows)
    qtile = 128

    seg_copy = pltpu.make_async_copy(seg_hbm, seg_ref, sem.at[1 + rows // tile])
    seg_copy.start()
    w_copy = pltpu.make_async_copy(wqkv_hbm, wqkv_ref, sem.at[0])
    w_copy.start()

    def tok_copy(t):
        at = pl.ds(pl.multiple_of(t * tile, tile), tile)
        return pltpu.make_async_copy(tok_hbm.at[at, :], tok_ref.at[at, :], sem.at[t + 1])

    for t in range(rows // tile):
        tok_copy(t).start()
    seg_copy.wait()
    seg = seg_ref[...]

    sub = iota((128, rows), 0)
    slot = sub % head_dim
    far = jnp.where(slot < slots, jnp.where(slot == seg, 0.0, FAR), 0.0)
    qm_s[...] = far.T.astype(BF16)
    half = iota((head_dim, rows), 0)
    onehot = jnp.where(half == seg, 1.0, 0.0).astype(BF16)
    for p in range(pairs):
        kt_s[2 * p, head_dim:, :] = onehot
        kt_s[2 * p + 1, :head_dim, :] = onehot

    starts = [0] + [jnp.sum((seg < s).astype(F32)).astype(I32) for s in range(1, slots)] + [rows]

    w_copy.wait()

    def project(t, _):
        tok_copy(t).wait()
        at = pl.ds(pl.multiple_of(t * tile, tile), tile)
        low = iota((tile, 128), 1) < head_dim
        x = tok_ref[at, :]
        qkv = jnp.dot(x, wqkv_ref[...], preferred_element_type=F32)
        q_s[at, :] = (qkv[:, :inner].astype(BF16) * head_dim**-0.5).astype(BF16)
        for p in range(pairs):
            k = qkv[:, inner + p * 128 : inner + (p + 1) * 128]
            kt = k.T.astype(BF16)
            kt_s[2 * p, :head_dim, at] = kt[:head_dim]
            kt_s[2 * p + 1, head_dim:, at] = kt[head_dim:]
            v = qkv[:, 2 * inner + p * 128 : 2 * inner + (p + 1) * 128]
            v_s[2 * p, at, :] = jnp.where(low, v, 1.0).astype(BF16)
            v_s[2 * p + 1, at, :] = jnp.where(low, 1.0, v).astype(BF16)
        return 0

    lax.fori_loop(0, rows // tile, project, 0)

    later = [
        pltpu.make_async_copy(wout_hbm, wout_ref, sem.at[2 + rows // tile]),
        pltpu.make_async_copy(wproj_hbm, wproj_ref, sem.at[3 + rows // tile]),
    ]
    for copy in later:
        copy.start()

    def window(tiles, span):
        low = iota((qtile, 128), 1) < head_dim
        scores = []
        for at, first in tiles:
            qm = qm_s[at, :]
            for n in range(HEADS):
                q = q_s[at, n // 2 * 128 : (n // 2 + 1) * 128]
                q = jnp.where(low, q, qm) if n % 2 == 0 else jnp.where(low, qm, q)
                scores.append(jnp.dot(q, kt_s[n, :, pl.ds(first, span)], preferred_element_type=F32))
        exps = [jnp.exp(s - jnp.max(s, axis=1, keepdims=True)).astype(BF16) for s in scores]
        outs = []
        for i, (at, first) in enumerate(tiles):
            for n in range(HEADS):
                outs.append(jnp.dot(exps[i * HEADS + n], v_s[n, pl.ds(first, span), :], preferred_element_type=F32))
        for i, (at, first) in enumerate(tiles):
            for p in range(pairs):
                even, odd = outs[i * HEADS + 2 * p], outs[i * HEADS + 2 * p + 1]
                top = jnp.where(low, even, odd)
                den = pltpu.roll(jnp.where(low, odd, even), head_dim, 1)
                ctx_ref[at, p * 128 : (p + 1) * 128] = (top / den).astype(BF16)

    group = 1

    def queries(t, _):
        los, width_needed = [], jnp.int32(0)
        for i in range(group):
            q0 = (t * group + i) * qtile
            lo = jnp.int32(0)
            hi = jnp.int32(rows)
            for s in range(1, slots):
                lo = jnp.where(starts[s] <= q0, starts[s], lo)
            for s in range(slots - 1, 0, -1):
                hi = jnp.where(starts[s] >= q0 + qtile, starts[s], hi)
            lo = lo // 128 * 128
            los.append(lo)
            width_needed = jnp.maximum(width_needed, hi - lo)
        spans = [w for w in (256, 384, 512, 640, 768, 896) if w < rows] + [rows]
        for below, w in zip([0] + spans, spans):

            @pl.when((width_needed > below) & (width_needed <= w))
            def _(w=w):
                tiles = []
                for i in range(group):
                    at = pl.ds(pl.multiple_of((t * group + i) * qtile, qtile), qtile)
                    tiles.append((at, 0 if w == rows else pl.multiple_of(jnp.minimum(los[i], rows - w), 128)))
                window(tiles, w)

        return 0

    lax.fori_loop(0, rows // (qtile * group), queries, 0)
    for copy in later:
        copy.wait()


def attend(seg, tokens, w_qkv, w_out, w_proj, slots):
    rows, width = tokens.shape
    inner = w_qkv.shape[1] // 3
    vmem = pl.BlockSpec(memory_space=pltpu.VMEM)
    hbm = pl.BlockSpec(memory_space=pltpu.HBM)
    return pl.pallas_call(
        functools.partial(attend_kernel, slots),
        name="attend",
        out_shape=[jax.ShapeDtypeStruct(x, BF16) for x in ((rows, inner), tokens.shape, w_out.shape, w_proj.shape)],
        in_specs=[hbm] * 5,
        out_specs=[vmem] * 4,
        scratch_shapes=[
            pltpu.VMEM((1, rows), I32),
            pltpu.VMEM((width, 3 * inner), BF16),
            pltpu.VMEM((rows, inner), BF16),
            pltpu.VMEM((HEADS, 128, rows), BF16),
            pltpu.VMEM((HEADS, rows, 128), BF16),
            pltpu.VMEM((rows, 128), BF16),
            pltpu.SemaphoreType.DMA((4 + rows // min(256, rows),)),
        ],
        compiler_params=pltpu.CompilerParams(vmem_limit_bytes=40 * 2**20),
        cost_estimate=pl.CostEstimate(flops=8 * 10**9, bytes_accessed=6 * 2**20, transcendentals=4 * 10**6),
    )(seg, tokens, w_qkv, w_out, w_proj)


def halves(x):
    hi = x.astype(BF16)
    return hi, (x - hi.astype(F32)).astype(BF16)


def loss_kernel(
    n_z, n_y, n_x, slots,
    counts_ref, pos_ref, seg_ref, tok_ref, ctx_ref, wout_ref, gain_ref, w_ref, loss_ref, grad_ref,
    mine_s, colp, rowp, drow, dcol, yrecv, ysend, mdr, mdc,
    p_s, unit_s, emb_s, wt_s,
    s_colp, r_colp, s_rowp, r_rowp, s_dr, r_dr, s_dc, r_dc, s_y, r_y,
):
    n_a, n_b = n_z * 2, n_y * n_x
    me = lax.axis_index("dp")
    core, b, z = me % 2, (me // 2) % n_b, me // (2 * n_b)
    a = z * 2 + core
    rows, width = tok_ref.shape
    embed = w_ref.shape[1]
    r_rows = slots * n_b
    c_cols = slots * n_a

    def ring(d, n):
        return min(d, n - d)

    row_peers = []
    for dy in range(n_y):
        for dx in range(n_x):
            o = (b // n_x + dy) % n_y * n_x + (b % n_x + dx) % n_x
            row_peers.append((2 * ring(dy, n_y) + 2 * ring(dx, n_x), o, z * (2 * n_b) + o * 2 + core))
    col_peers = []
    for dz in range(n_z):
        for dc in range(2):
            o = (z + dz) % n_z * 2 + (core + dc) % 2
            col_peers.append((2 * ring(dz, n_z) + dc, o, (o // 2) * (2 * n_b) + b * 2 + o % 2))
    row_peers, col_peers = row_peers[1:], col_peers[1:]

    barrier = pltpu.get_barrier_semaphore()
    for _, _, device in row_peers + col_peers:
        pl.semaphore_signal(barrier, inc=1, device_id=(device,), device_id_type=MESH)

    def exchange(peers, mine, source, dest, send, recv):
        out = []
        for k, (hops, o, device) in enumerate(peers):
            out.append((
                hops,
                functools.partial(
                    pltpu.make_async_remote_copy, src_ref=source(o), dst_ref=dest.at[mine], send_sem=send.at[k],
                    recv_sem=recv.at[mine], device_id=(device,), device_id_type=MESH,
                ),
                functools.partial(
                    pltpu.make_async_remote_copy, src_ref=source(o), dst_ref=dest.at[o], send_sem=send.at[k],
                    recv_sem=recv.at[o], device_id=(device,), device_id_type=MESH,
                ),
            ))
        return sorted(out, key=lambda c: -c[0])

    def start(*exchanges):
        for _, copy, _ in sorted(sum(exchanges, []), key=lambda c: -c[0]):
            copy().start()

    def arrive(exchange):
        for _, _, copy in reversed(exchange):
            copy().wait_recv()

    x_col = exchange(col_peers, a, lambda o: mine_s, colp, s_colp, r_colp)
    x_row = exchange(row_peers, b, lambda o: mine_s, rowp, s_rowp, r_rowp)
    x_dr = exchange(row_peers, b, lambda o: mdr, drow, s_dr, r_dr)
    x_dc = exchange(col_peers, a, lambda o: mdc, dcol, s_dc, r_dc)
    x_y = exchange(row_peers, b, lambda o: ysend.at[o], yrecv, s_y, r_y)

    s_id = iota((slots, 1), 0)
    lane = iota((slots, 128), 1)
    n_devices = counts_ref.shape[1]
    my_count = jnp.sum(jnp.where(iota((1, n_devices), 1) == me, counts_ref[...], 0).astype(F32), axis=1, keepdims=True)
    live_own = (s_id.astype(F32) < my_count).astype(F32)
    diagonal = iota((slots, slots), 0) == iota((slots, slots), 1)

    def down(values):
        return jnp.sum(jnp.where(diagonal, values.astype(F32), 0.0), axis=1, keepdims=True)

    places = pos_ref[...]
    side = jnp.where(lane == 0, down(places >> 5), jnp.where(lane == 1, down(places & 31), 0.0))
    side = jnp.where(lane == 2, live_own, side)
    mine_s[:, width:] = side.astype(BF16)

    tile = min(256, rows)

    def mix_in(t):
        at = pl.ds(t * tile, tile)
        return tok_ref[at, :].astype(F32) + jnp.dot(ctx_ref[at, :], wout_ref[...], preferred_element_type=F32)

    def norm(resid):
        centre = resid - jnp.sum(resid, axis=1, keepdims=True) * (1.0 / width)
        variance = jnp.sum(centre * centre, axis=1, keepdims=True) * (1.0 / width)
        return (centre * lax.rsqrt(variance + 1e-05) * gain_ref[...]).astype(BF16)

    def pool(t, hidden):
        member = (iota((16, tile), 0) == seg_ref[:, pl.ds(t * tile, tile)]).astype(F32).astype(BF16)
        return jnp.dot(member, hidden, preferred_element_type=F32)

    resids = [mix_in(t) for t in range(rows // tile)]
    sums = sum(pool(t, norm(resid)) for t, resid in enumerate(resids))
    sizes = jnp.sum((iota((16, rows), 0) == seg_ref[...]).astype(F32), axis=1, keepdims=True)
    pooled = (sums[:slots] / sizes[:slots]).astype(BF16)
    mine_s[:, :width] = pooled

    pl.semaphore_wait(barrier, n_a + n_b - 2)
    start(x_col, x_row)

    proj = jnp.dot(pooled, w_ref[...], preferred_element_type=F32)
    rnorm = lax.rsqrt(jnp.sum(proj * proj, axis=1, keepdims=True) + 1e-06)
    unit_s[...] = proj * rnorm

    def turn(j, _):
        at = pl.ds(pl.multiple_of(j * 128, 128), 128)
        wt_s[at, :] = w_ref[:, at].T
        return 0

    lax.fori_loop(0, embed // 128, turn, 0)
    colp[a] = mine_s[...]
    rowp[b] = mine_s[...]
    p_s[...] = jnp.zeros_like(p_s)
    arrive(x_row)
    for o in range(n_b):
        p_s[128 + o * slots : 128 + (o + 1) * slots, :] = rowp[o].astype(F32)
    arrive(x_col)
    for o in range(n_a):
        p_s[o * slots : (o + 1) * slots, :] = colp[o].astype(F32)

    proj_all = jnp.dot(p_s[:, :width].astype(BF16), w_ref[...], preferred_element_type=F32)
    rnorm_all = lax.rsqrt(jnp.sum(proj_all * proj_all, axis=1, keepdims=True) + 1e-06)
    emb_s[...] = (proj_all * rnorm_all).astype(BF16)
    emb_j = emb_s[:128, :]
    logits = SCALE * lax.dot_general(emb_s[128 : 128 + r_rows, :], emb_j, NT, preferred_element_type=F32)

    r = iota((r_rows, 128), 0)
    c = iota((r_rows, 128), 1)
    id_i = (z * (2 * n_b) + (r // slots) * 2 + core) * slots + r % slots
    o_j = c // slots
    id_j = ((o_j // 2) * (2 * n_b) + b * 2 + o_j % 2) * slots + c % slots
    eye = r == c
    square = iota((128, 128), 0) == iota((128, 128), 1)

    def along(column):
        return jnp.sum(jnp.where(square, column, 0.0), axis=0, keepdims=True)

    side_j = p_s[:128, width:]
    side_i = p_s[128 : 128 + r_rows, width:]
    pos_i, live_i = side_i[:, 0:1] * 32.0 + side_i[:, 1:2], side_i[:, 2:3] > 0.5
    pos_j, live_j = along(side_j[:, 0:1] * 32.0 + side_j[:, 1:2]), along(side_j[:, 2:3]) > 0.5
    inside = (c < c_cols) & (id_i != id_j)
    expd = jnp.exp(logits)
    exp_j = jnp.where(inside & live_i, expd, 0.0)
    mdc[...] = jnp.sum(exp_j, axis=0, keepdims=True)
    start(x_dc)
    exp_i = jnp.where(inside & live_j, expd, 0.0)
    hit_i = (pos_i == id_j.astype(F32)) & (c < c_cols)
    hit_j = (pos_j == id_i.astype(F32)) & (c < c_cols)
    part_i = jnp.sum(exp_i, axis=1, keepdims=True)
    picked = jnp.sum(jnp.where(hit_i, logits, 0.0), axis=1, keepdims=True)
    mdr[0:1, :] = jnp.sum(jnp.where(eye, part_i, 0.0), axis=0, keepdims=True)
    mdr[1:2, :] = jnp.sum(jnp.where(eye, picked, 0.0), axis=0, keepdims=True)
    start(x_dr)
    drow[b] = mdr[...]
    dcol[a] = mdc[...]
    arrive(x_dr)
    arrive(x_dc)
    sums_i = jnp.sum(drow[...], axis=0)
    den_j = jnp.sum(dcol[...], axis=0)
    den_i = jnp.sum(jnp.where(eye, sums_i[0:1], 0.0), axis=1, keepdims=True)
    w_i = jnp.where(live_i, exp_i / den_i - hit_i.astype(F32), 0.0)
    den_j = jnp.where(den_j > 0.0, den_j, 1.0)
    w_j = jnp.where(live_j & (c < c_cols), exp_j / den_j - hit_j.astype(F32), 0.0)
    mix = jnp.concatenate(halves(w_i + w_j), axis=0)
    y = jnp.dot(mix, emb_j, preferred_element_type=F32)
    y = (y[:r_rows] + y[r_rows:]).astype(BF16)
    for o in range(n_b):
        ysend[o] = y[o * slots : (o + 1) * slots]
    start(x_y)
    yrecv[b] = ysend[b]

    table = jnp.log(sums_i[0:1]) - sums_i[1:2]
    mine = jnp.sum(jnp.where(lane == b * slots + iota((slots, 128), 0), table, 0.0), axis=1, keepdims=True)
    mine = jnp.where(live_own > 0.5, mine, 0.0)
    loss_lane = jnp.sum(jnp.where(lane == iota((slots, 128), 0), mine, 0.0), axis=0, keepdims=True)
    loss_ref[...] = loss_lane[:, :slots]

    arrive(x_y)
    d_emb = SCALE * jnp.sum(yrecv[...].astype(F32), axis=0)
    own = unit_s[...]
    radial = jnp.sum(d_emb * own, axis=1, keepdims=True)
    d_proj = ((d_emb - radial * own) * rnorm).astype(BF16)
    grad_ref[...] = jnp.dot(d_proj, wt_s[...], preferred_element_type=F32)
    for x in (x_col, x_row, x_dr, x_dc, x_y):
        for _, copy, _ in x:
            copy().wait_send()


def contrast(counts, positives, seg, tokens, ctx, w_out, gain, w_proj, n_z, n_y, n_x):
    slots = positives.shape[1]
    n_a, n_b = n_z * 2, n_y * n_x
    width, embed = w_proj.shape
    vmem = pl.BlockSpec(memory_space=pltpu.VMEM)
    sems = [pltpu.SemaphoreType.DMA((n,)) for n in (n_a, n_b, n_b, n_a, n_b) for _ in range(2)]
    return pl.pallas_call(
        functools.partial(loss_kernel, n_z, n_y, n_x, slots),
        name="contrast",
        out_shape=(jax.ShapeDtypeStruct((1, slots), F32), jax.ShapeDtypeStruct((slots, width), F32)),
        in_specs=[vmem] * 8,
        out_specs=(vmem, vmem),
        scratch_shapes=[
            pltpu.VMEM((slots, width + 128), BF16),
            pltpu.VMEM((n_a, slots, width + 128), BF16),
            pltpu.VMEM((n_b, slots, width + 128), BF16),
            pltpu.VMEM((n_b, 2, 128), F32),
            pltpu.VMEM((n_a, 1, 128), F32),
            pltpu.VMEM((n_b, slots, embed), BF16),
            pltpu.VMEM((n_b, slots, embed), BF16),
            pltpu.VMEM((2, 128), F32),
            pltpu.VMEM((1, 128), F32),
            pltpu.VMEM((128 + slots * n_b, width + 128), F32),
            pltpu.VMEM((slots, embed), F32),
            pltpu.VMEM((128 + slots * n_b, embed), BF16),
            pltpu.VMEM((embed, width), BF16),
            *sems,
        ],
        compiler_params=pltpu.CompilerParams(collective_id=0, has_side_effects=True, vmem_limit_bytes=40 * 2**20),
    )(counts, positives, seg, tokens, ctx, w_out, gain, w_proj)


def deliver_kernel(loss_ref, grad_ref, loss_hbm, grad_hbm, sem):
    copies = [pltpu.make_async_copy(loss_ref, loss_hbm, sem.at[0]), pltpu.make_async_copy(grad_ref, grad_hbm, sem.at[1])]
    for copy in copies:
        copy.start()
    for copy in copies:
        copy.wait()


def deliver(loss, grad):
    vmem = pl.BlockSpec(memory_space=pltpu.VMEM)
    hbm = pl.BlockSpec(memory_space=pltpu.HBM)
    return pl.pallas_call(
        deliver_kernel,
        name="deliver",
        out_shape=(jax.ShapeDtypeStruct(loss.shape, F32), jax.ShapeDtypeStruct(grad.shape, F32)),
        in_specs=[vmem, vmem],
        out_specs=(hbm, hbm),
        scratch_shapes=[pltpu.SemaphoreType.DMA((2,))],
        compiler_params=pltpu.CompilerParams(vmem_limit_bytes=2**20),
    )(loss, grad)


def body(grid, tokens, seg_ids, counts, positives, w_qkv, w_out, ln_gain, w_proj):
    slots = positives.shape[0]
    in_hbm = functools.partial(pltpu.with_memory_space_constraint, memory_space=pltpu.HBM)
    ctx, tokens, w_out, w_proj = attend(*map(in_hbm, (seg_ids, tokens, w_qkv, w_out, w_proj)), slots)
    loss, grad = contrast(counts[None, :], positives[None, :], seg_ids, tokens, ctx, w_out, ln_gain[None, :], w_proj, *grid)
    loss, grad = deliver(loss, grad)
    return loss.reshape(slots), grad


def solution(mesh):
    grid = (mesh.size // 32, 4, 4)
    return jax.shard_map(
        functools.partial(body, grid),
        mesh=mesh,
        in_specs=(P("dp", None), P("dp", None), P(), P("dp"), P(), P(), P(), P()),
        out_specs=(P("dp"), P("dp", None)),
        check_vma=False,
    )
```
